128 devices in a mesh: pts: 16 (over y, z_lo, core), freq: 8 (over z_hi, x).
Axes of the slice: x: 4, y: 4, z: 4 (z_hi: 2, z_lo: 2; z = z_hi * 2 + z_lo), core: 2. Of those that a mesh axis runs over, the one named last changes fastest.
Arguments:
- spectra: bfloat16 [128, 2, 32, 32768], P('freq', None, None, 'pts'), may hold values from -6 to 6
- weights: float32 [32768], P('pts'), may hold values from 0.25 to 4
- triads: int32 [128, 2], replicated, may hold values from 0 to 127, as said below
Outputs:
- bispectrum: float32 [128, 2, 32, 32], P('freq')
- density: float32 [128, 2, 32, 32], P('freq')
- vectors: float32 [128, 2, 32], P('freq')
- energy: float32 [128], P('freq')
- mode_fields: float32 [128, 2, 32768], P('freq', None, 'pts')
The draws below stay inside these ranges and needn't reach their ends.
Inputs may be any that keep to these rules, and one draw needn't show every extreme that they name: Row t holds (k, l) of triad t. The triads of group g, rows g * 16 to (g + 1) * 16 - 1, have k within the group's own frequencies g * 16 to (g + 1) * 16 - 1. The l of exactly 2 triads of each group lie in each group's frequency range. Among the 32 frequencies l and (k + l) mod 128 of one group's triads, at most 6 lie in any one group's range, and in every group some range holds exactly 6.
All inputs are finite; a program needn't handle non-finite values.
Results may differ from the reference program's by a relative error of at most 0.0052.
Values may be sent and summed in bfloat16 or wider, within the bound.
No kernel may reach another device: no remote copies, remote signals or barrier semaphores. Data moves between devices by JAX's collectives and lax.ppermute only.
A program may use at most 128 MiB of HBM per device.

```python
import math
import jax
import jax.numpy as jnp
from jax import lax

F = 128
NB = 32
TRI_G = 16
ITERS = 3
NPTS = 32768
N_FREQ = 8


def draw_triads(key, part):
    f_dev = F // N_FREQ
    key_list = jax.random.split(jax.random.fold_in(key, 11), 7)
    group_ids = jnp.arange(N_FREQ, dtype=jnp.int32)[:, None]
    base_owner = jnp.arange(TRI_G, dtype=jnp.int32) % N_FREQ

    def shuffle_owner(subkey):
        return jax.random.permutation(subkey, base_owner)
    owner_l = jax.vmap(shuffle_owner)(jax.random.split(key_list[0], N_FREQ)).astype(jnp.int32)
    target = jax.random.randint(key_list[1], (N_FREQ, 1), 0, N_FREQ, dtype=jnp.int32)
    coin_flip = jax.random.randint(key_list[2], (N_FREQ, TRI_G), 0, 2, dtype=jnp.int32)
    before_target = (target + N_FREQ - 1) % N_FREQ
    carry_bit = jnp.where(owner_l == target, 0, jnp.where(owner_l == before_target, 1, coin_flip))
    low_k = jax.random.randint(key_list[3], (N_FREQ, TRI_G), 0, f_dev, dtype=jnp.int32)
    high_k = jax.random.randint(key_list[4], (N_FREQ, TRI_G), 1, f_dev, dtype=jnp.int32)
    rest_k = jnp.where(carry_bit == 1, high_k, low_k)
    lower_end = jnp.where(carry_bit == 1, f_dev - rest_k, 0)
    upper_end = jnp.where(carry_bit == 1, f_dev, f_dev - rest_k)
    rest_l = jax.random.randint(key_list[5], (N_FREQ, TRI_G), lower_end, upper_end, dtype=jnp.int32)
    freq_first = group_ids * f_dev + rest_k
    freq_second = owner_l * f_dev + rest_l
    return jnp.stack([freq_first, freq_second], axis=-1).reshape(N_FREQ * TRI_G, 2).astype(jnp.int32)


def shard_levels(stream_key, dims, cuts, least, high):
    def one(position, shards_of):
        steps = jax.random.uniform(jax.random.fold_in(jax.random.fold_in(stream_key, 6), position), (shards_of,), jnp.float32, least / len(cuts), high / len(cuts))
        return jnp.repeat(jnp.exp(steps), dims[position] // shards_of).reshape((-1,) + (1,) * (len(dims) - position - 1))

    factor_of = one(*cuts[0])
    for cut in cuts[1:]:
        factor_of = factor_of * one(*cut)
    return factor_of


def scatter_about(own_key, shape, spread, most, cuts=(), held_as=jnp.bfloat16):
    drawn = spread * jax.random.normal(own_key, shape, jnp.float32)
    if cuts:
        drawn = drawn * shard_levels(own_key, shape, cuts, -0.22, 0.18)
    return jnp.clip(drawn, -most, most).astype(held_as)


def setup_inputs(seed: int = 0) -> dict:
    keys = jax.random.split(jax.random.key(seed), 4)
    spectra = scatter_about(keys[0], (F, 2, NB, NPTS), 1.0, 6.0, ((0, 8), (3, 16)))
    weights = jnp.clip(jnp.exp(math.log(4.0) - 2.7725887 * jax.random.uniform(keys[1], (NPTS,), jnp.float32) ** shard_levels(keys[1], (NPTS,), ((0, 16),), -0.2, 0.2)), 0.25, 4.0)
    triads = draw_triads(jax.random.fold_in(keys[3], 71), 0)
    return {"spectra": spectra, "weights": weights, "triads": triads}


highest = lax.Precision.HIGHEST

def pair_gram(left, right):
    half_rows = left.shape[1]
    flat_left = left.reshape(2 * half_rows, left.shape[2])
    flat_right = right.reshape(2 * half_rows, right.shape[2])
    joined = jnp.dot(flat_left, flat_right.T, preferred_element_type=jnp.float32)
    real_part = joined[:half_rows, :half_rows] + joined[half_rows:, half_rows:]
    imag_part = joined[:half_rows, half_rows:] - joined[half_rows:, :half_rows]
    return jnp.stack([real_part, imag_part])

def weighted_product(first_rows, second_rows, weights):
    first_real = first_rows[0].astype(jnp.float32)
    first_imag = first_rows[1].astype(jnp.float32)
    second_real = second_rows[0].astype(jnp.float32)
    second_imag = second_rows[1].astype(jnp.float32)
    prod_real = first_real * second_real - first_imag * second_imag
    prod_imag = first_real * second_imag + first_imag * second_real
    return (jnp.stack([prod_real, prod_imag]) * weights).astype(jnp.bfloat16)

def apply_matrix(matrix, vector):
    return jnp.einsum('...ab,...b->...a', matrix, vector, precision=highest)

def apply_adjoint(matrix, vector):
    return jnp.einsum('...ba,...b->...a', matrix, vector, precision=highest)

def power_iteration(bispec):
    real_mat = bispec[..., 0, :, :]
    imag_mat = bispec[..., 1, :, :]
    order = real_mat.shape[-1]
    vec_real = jnp.full(real_mat.shape[:-1], 1.0 / math.sqrt(order), jnp.float32)
    vec_imag = jnp.zeros(real_mat.shape[:-1], jnp.float32)
    for sweep_index in range(ITERS):
        out_real = apply_matrix(real_mat, vec_real) - apply_matrix(imag_mat, vec_imag)
        out_imag = apply_matrix(real_mat, vec_imag) + apply_matrix(imag_mat, vec_real)
        back_real = apply_adjoint(real_mat, out_real) + apply_adjoint(imag_mat, out_imag)
        back_imag = apply_adjoint(real_mat, out_imag) - apply_adjoint(imag_mat, out_real)
        factor = 1.0 / jnp.sqrt(lax.optimization_barrier(jnp.sum(back_real * back_real + back_imag * back_imag, axis=-1)) + 1.0)
        vec_real = back_real * factor[..., None]
        vec_imag = back_imag * factor[..., None]
    out_real = apply_matrix(real_mat, vec_real) - apply_matrix(imag_mat, vec_imag)
    out_imag = apply_matrix(real_mat, vec_imag) + apply_matrix(imag_mat, vec_real)
    top_part = lax.optimization_barrier(jnp.sum(out_real * out_real + out_imag * out_imag, axis=-1))
    bottom_part = order * (lax.optimization_barrier(jnp.sum(vec_real * vec_real + vec_imag * vec_imag, axis=-1)) + 1.0)
    return (jnp.stack([vec_real, vec_imag], axis=-2), top_part / bottom_part)

def reference(spectra, weights, triads):
    point_count = spectra.shape[-1]
    blocks = spectra.shape[2]
    k_index = triads[:, 0].astype(jnp.int32)
    l_index = triads[:, 1].astype(jnp.int32)
    m_index = ((k_index + l_index) % F).astype(jnp.int32)

    def one_triad(indices):
        first_rows = lax.dynamic_index_in_dim(spectra, indices[0], 0, keepdims=False)
        second_rows = lax.dynamic_index_in_dim(spectra, indices[1], 0, keepdims=False)
        third_rows = lax.dynamic_index_in_dim(spectra, indices[2], 0, keepdims=False)
        return pair_gram(weighted_product(first_rows, second_rows, weights), third_rows)
    raw_sums = lax.map(one_triad, (k_index, l_index, m_index))
    bispectrum = raw_sums * (1.0 / math.sqrt(blocks * point_count))

    def one_freq(rows):
        weighted = (rows.astype(jnp.float32) * weights).astype(jnp.bfloat16)
        return pair_gram(weighted, rows)
    density = lax.map(one_freq, spectra) * (1.0 / point_count)
    vectors, energy = power_iteration(bispectrum)
    vector_low = vectors.astype(jnp.bfloat16)

    def one_mode(inputs):
        third_rows = lax.dynamic_index_in_dim(spectra, inputs[0], 0, keepdims=False)
        mixed = jnp.einsum('cbp,db->cdp', third_rows.astype(jnp.float32), inputs[1].astype(jnp.float32), precision=highest)
        return jnp.stack([mixed[0, 0] - mixed[1, 1], mixed[0, 1] + mixed[1, 0]])
    mode_fields = lax.map(one_mode, (m_index, vector_low))
    return (bispectrum, density, vectors, energy, mode_fields)
```

```python
import math

import jax
import jax.numpy as jnp
from jax import lax
from jax.experimental import pallas as pl
from jax.experimental.pallas import tpu as pltpu
from jax.sharding import PartitionSpec as P

ITERS = 3
EVERYONE = ("pts", "freq")
NT = (((1,), (1,)), ((), ()))
VMEM = pl.BlockSpec(memory_space=pltpu.VMEM)
SMEM = pl.BlockSpec(memory_space=pltpu.SMEM)


def gram(left_re, left_im, right):
    half = right.shape[0] // 2
    right_re, right_im = right[:half], right[half:]
    turned = jnp.concatenate([right_im, -right_re], axis=0)
    return lax.dot_general(
        left_re, right, NT, preferred_element_type=jnp.float32
    ) + lax.dot_general(left_im, turned, NT, preferred_element_type=jnp.float32)


def folded(matrix):
    half = matrix.shape[0] // 2
    return jnp.concatenate([matrix[:half], matrix[half:]], axis=1)


def density_kernel(spectra_ref, weights_ref, out_ref):
    rows = spectra_ref[0]
    half = rows.shape[0] // 2
    weighted = (rows.astype(jnp.float32) * weights_ref[...]).astype(jnp.bfloat16)
    out_ref[0] = folded(gram(weighted[:half], weighted[half:], rows))


def density_parts(spectra, weights):
    freqs, _, blocks, points = spectra.shape
    return pl.pallas_call(
        density_kernel,
        grid=(freqs,),
        in_specs=[
            pl.BlockSpec((1, 2 * blocks, points), lambda f: (f, 0, 0)),
            pl.BlockSpec((1, points), lambda f: (0, 0)),
        ],
        out_specs=pl.BlockSpec((1, blocks // 2, 4 * blocks), lambda f: (f, 0, 0)),
        out_shape=jax.ShapeDtypeStruct((freqs, blocks // 2, 4 * blocks), jnp.float32),
        cost_estimate=pl.CostEstimate(
            flops=freqs * 4 * blocks * blocks * points * 2,
            bytes_accessed=spectra.size * 2,
            transcendentals=0,
        ),
        name="density",
    )(spectra.reshape(freqs, 2 * blocks, points), weights.reshape(1, points))


def triad_kernel(groups, triads_ref, spectra_ref, weights_ref, out_ref):
    total = spectra_ref.shape[0]
    half = spectra_ref.shape[1] // 2
    count = out_ref.shape[0]
    per_group = count // groups

    def step(j, carry):
        t = lax.rem(j, groups) * per_group + lax.div(j, groups)
        k = triads_ref[2 * t]
        l = triads_ref[2 * t + 1]
        m = lax.rem(k + l, total)
        first = spectra_ref[k].astype(jnp.float32)
        second = spectra_ref[l].astype(jnp.float32)
        weights = weights_ref[...]
        ar, ai, br, bi = first[:half], first[half:], second[:half], second[half:]
        re = ((ar * br - ai * bi) * weights).astype(jnp.bfloat16)
        im = ((ar * bi + ai * br) * weights).astype(jnp.bfloat16)
        out_ref[j] = folded(gram(re, im, spectra_ref[m]))
        return carry

    lax.fori_loop(0, count, step, 0, unroll=4)


def triad_parts(triads, spectra, weights, groups):
    count = triads.shape[0]
    total, rows, points = spectra.shape
    return pl.pallas_call(
        lambda *refs: triad_kernel(groups, *refs),
        in_specs=[SMEM, VMEM, VMEM],
        out_specs=VMEM,
        out_shape=jax.ShapeDtypeStruct((count, rows // 4, 2 * rows), jnp.float32),
        cost_estimate=pl.CostEstimate(
            flops=count * rows * rows * points * 2,
            bytes_accessed=spectra.size * 2,
            transcendentals=0,
        ),
        name="triads",
    )(triads.reshape(-1), spectra, weights)


def power_kernel(scale, parts_ref, matrix_ref, vector_ref):
    total = jnp.sum(parts_ref[...], axis=0) * scale
    matrix_ref[...] = total
    blocks = 2 * total.shape[0]
    lane = lax.broadcasted_iota(jnp.int32, (1, 4 * blocks), 1)
    lower = lane < 2 * blocks
    other = pltpu.roll(total, 2 * blocks, 1)
    both = jnp.concatenate(
        [jnp.where(lower, total, other), jnp.where(lower, other, total)], axis=0
    )
    sign = jnp.where(lax.rem(lax.div(lane, blocks), 2) == 0, 1.0, -1.0)

    def forward(one, two):
        re = jnp.sum(both * jnp.where(lower, one, 0.0), axis=1, keepdims=True)
        im = jnp.sum(both * jnp.where(lower, two, 0.0), axis=1, keepdims=True)
        return re, im

    def square(one):
        return jnp.sum(jnp.where(lower, one * one, 0.0), axis=1, keepdims=True)

    start = 1.0 / math.sqrt(blocks)
    one = jnp.where(sign > 0, start, 0.0)
    two = jnp.where(sign > 0, 0.0, start)
    for _ in range(ITERS):
        re, im = forward(one, two)
        with_re = jnp.sum(both * re, axis=0, keepdims=True)
        with_im = jnp.sum(both * im, axis=0, keepdims=True)
        one = with_re + sign * pltpu.roll(with_im, blocks, 1)
        two = with_im - sign * pltpu.roll(with_re, blocks, 1)
        factor = 1.0 / jnp.sqrt(square(one) + 1.0)
        one = one * factor
        two = two * factor
    re, im = forward(one, two)
    top = jnp.sum(re * re + im * im, axis=0, keepdims=True)
    energy = top / (blocks * (square(one) + 1.0))
    row = jnp.where(lower, one * sign, energy)
    vector_ref[...] = jnp.broadcast_to(row[None], vector_ref.shape)


def power(parts, scale):
    count, rows, lanes = parts.shape
    return pl.pallas_call(
        lambda *refs: power_kernel(scale, *refs),
        in_specs=[VMEM],
        out_specs=[VMEM, VMEM],
        out_shape=[
            jax.ShapeDtypeStruct((rows, lanes), jnp.float32),
            jax.ShapeDtypeStruct((count, 1, lanes), jnp.float32),
        ],
        name="power",
    )(parts)


def modes_kernel(triads_ref, spectra_ref, vectors_ref, out_ref):
    total = spectra_ref.shape[0]
    steps = vectors_ref.shape[0]
    rows = vectors_ref.shape[1]
    each = rows // 2

    def step(s, carry):
        picked = []
        for q in range(each):
            t = s * each + q
            m = lax.rem(triads_ref[2 * t] + triads_ref[2 * t + 1], total)
            picked.append(spectra_ref[m])
        right = jnp.concatenate(picked, axis=0)
        out_ref[s] = jnp.dot(vectors_ref[s], right, preferred_element_type=jnp.float32)
        return carry

    lax.fori_loop(0, steps, step, 0, unroll=2)


def modes(triads, spectra, vectors):
    count, width = vectors.shape
    total, rows, points = spectra.shape
    half = width // 2
    each = 4
    re, im = vectors[:, :half], vectors[:, half:]
    pair = jnp.stack([re, -im, im, re], axis=1).reshape(count // each, each, 2, 1, width)
    own = jnp.eye(each, dtype=jnp.bfloat16).reshape(1, each, 1, each, 1)
    left = (pair * own).reshape(count // each, 2 * each, each * width)
    return pl.pallas_call(
        modes_kernel,
        in_specs=[SMEM, VMEM, VMEM],
        out_specs=VMEM,
        out_shape=jax.ShapeDtypeStruct((count // each, 2 * each, points), jnp.float32),
        cost_estimate=pl.CostEstimate(
            flops=count * rows * points * 4,
            bytes_accessed=spectra.size * 2,
            transcendentals=0,
        ),
        name="modes",
    )(triads.reshape(-1), spectra, left)


def to_all(value, axis):
    length = lax.axis_size(axis)
    return lax.all_to_all(
        jnp.broadcast_to(value[None], (length, *value.shape)), axis, 0, 0, tiled=True
    )


def unfolded(packed):
    n, half, lanes = packed.shape
    blocks = 2 * half
    parted = packed.reshape(n, half, 2, 2, blocks)
    return parted.transpose(0, 3, 2, 1, 4).reshape(n, 2, blocks, blocks)


def local(spectra, weights, triads):
    groups = lax.axis_size("freq")
    lines = lax.axis_size("pts")
    group = lax.axis_index("freq")
    f_dev, _, blocks, points = spectra.shape
    per_group = triads.shape[0] // groups
    point_count = points * lines
    share = points // groups

    send = spectra.reshape(f_dev, 2, blocks, groups, share).transpose(3, 0, 1, 2, 4)
    turned = lax.all_to_all(send, "freq", 0, 0, tiled=True)
    turned = turned.reshape(groups * f_dev, 2 * blocks, share)
    own_weights = lax.dynamic_slice_in_dim(weights, group * share, share, 0).reshape(1, share)

    dens_parts = density_parts(spectra, weights)
    dens_own = jnp.sum(lax.all_to_all(dens_parts, "pts", 0, 0, tiled=True), axis=0)
    dens_own = dens_own * (1.0 / point_count)

    parts = triad_parts(triads, turned, own_weights, groups)
    parts = lax.all_to_all(parts, EVERYONE, 0, 0, tiled=True)
    matrix, vector = power(parts, 1.0 / math.sqrt(blocks * point_count))

    rows = lax.all_to_all(vector, EVERYONE, 0, 0, tiled=True)
    rows = rows.reshape(lines, groups, -1).swapaxes(0, 1)
    vectors = rows[:, :, : 2 * blocks].reshape(groups * per_group, 2 * blocks)
    fields = modes(triads, turned, vectors.astype(jnp.bfloat16))
    fields = fields.reshape(groups, 2 * per_group, share)
    fields = lax.all_to_all(fields, "freq", 0, 0, tiled=True)
    mode_fields = fields.swapaxes(0, 1).reshape(per_group, 2, points)

    both = to_all(jnp.concatenate([matrix, dens_own], axis=0), "pts")
    bispectrum = unfolded(both[:, : blocks // 2])
    density = unfolded(both[:, blocks // 2 :])

    own = lax.dynamic_index_in_dim(rows, group, 0, keepdims=False)
    out_vectors = own[:, : 2 * blocks].reshape(per_group, 2, blocks)
    energy = own[:, 2 * blocks]
    return (bispectrum, density, out_vectors, energy, mode_fields)


def solution(mesh):
    in_specs = (P("freq", None, None, "pts"), P("pts"), P())
    out_specs = (
        P("freq", None, None, None),
        P("freq", None, None, None),
        P("freq", None, None),
        P("freq"),
        P("freq", None, "pts"),
    )
    return jax.shard_map(local, mesh=mesh, in_specs=in_specs, out_specs=out_specs, check_vma=False)
```

```python
import math

import jax
import jax.numpy as jnp
from jax import lax
from jax.experimental import pallas as pl
from jax.experimental.pallas import tpu as pltpu
from jax.sharding import Mesh
from jax.sharding import PartitionSpec as P

ITERS = 3
EACH = 4
NT = (((1,), (1,)), ((), ()))
VMEM = pl.BlockSpec(memory_space=pltpu.VMEM)
SMEM = pl.BlockSpec(memory_space=pltpu.SMEM)


def params(mib=12):
    return pltpu.CompilerParams(vmem_limit_bytes=mib << 20)


def gram(left_re, left_im, right):
    half = right.shape[0] // 2
    right_re, right_im = right[:half], right[half:]
    turned = jnp.concatenate([right_im, -right_re], axis=0)
    return lax.dot_general(
        left_re, right, NT, preferred_element_type=jnp.float32
    ) + lax.dot_general(left_im, turned, NT, preferred_element_type=jnp.float32)


def folded(matrix):
    half = matrix.shape[0] // 2
    return jnp.concatenate([matrix[:half], matrix[half:]], axis=1)


def cut_kernel(rows_ref, out_ref, sems):
    count, _, share = out_ref.shape
    copies = [
        pltpu.make_async_copy(
            rows_ref.at[:, pl.ds(d * share, share)], out_ref.at[d], sems.at[d]
        )
        for d in range(count)
    ]
    for copy in copies:
        copy.start()
    for copy in copies:
        copy.wait()


def cut(rows, count):
    length, points = rows.shape
    return pl.pallas_call(
        cut_kernel,
        in_specs=[pl.BlockSpec(memory_space=pl.ANY)],
        out_specs=VMEM,
        out_shape=pltpu.VMEM((count, length, points // count), rows.dtype),
        scratch_shapes=[pltpu.SemaphoreType.DMA((count,))],
        compiler_params=params(),
        name="cut",
    )(rows)


def density_kernel(spectra_ref, weights_ref, out_ref):
    half = spectra_ref.shape[1] // 2
    for f in range(spectra_ref.shape[0]):
        rows = spectra_ref[f]
        weighted = (rows.astype(jnp.float32) * weights_ref[...]).astype(jnp.bfloat16)
        out_ref[f] = folded(gram(weighted[:half], weighted[half:], rows))


def density_parts(spectra, weights):
    freqs, rows, points = spectra.shape
    return pl.pallas_call(
        density_kernel,
        grid=(freqs // EACH,),
        in_specs=[
            pl.BlockSpec((EACH, rows, points), lambda f: (f, 0, 0)),
            pl.BlockSpec((1, points), lambda f: (0, 0)),
        ],
        out_specs=pl.BlockSpec((EACH, rows // 4, 2 * rows), lambda f: (f, 0, 0)),
        out_shape=jax.ShapeDtypeStruct((freqs, rows // 4, 2 * rows), jnp.float32),
        cost_estimate=pl.CostEstimate(
            flops=freqs * rows * rows * points * 2,
            bytes_accessed=spectra.size * 2,
            transcendentals=0,
        ),
        compiler_params=params(24),
        name="density",
    )(spectra, weights)


def triad_kernel(groups, mine, triads_ref, spectra_ref, weights_ref, out_ref):
    total, rows, share = spectra_ref.shape
    half = rows // 2
    count = out_ref.shape[0]
    per_group = 2 * count // groups
    core = lax.axis_index("core")
    core = core if mine else 1 - core
    offset = pl.multiple_of(lax.axis_index("freq") * share, share)

    def step(j, carry):
        t = lax.rem(j, groups) * per_group + 2 * lax.div(j, groups) + core
        k = triads_ref[0, t]
        l = triads_ref[1, t]
        m = lax.rem(k + l, total)
        first = spectra_ref[k].astype(jnp.float32)
        second = spectra_ref[l].astype(jnp.float32)
        weights = weights_ref[:, pl.ds(offset, share)]
        ar, ai, br, bi = first[:half], first[half:], second[:half], second[half:]
        re = ((ar * br - ai * bi) * weights).astype(jnp.bfloat16)
        im = ((ar * bi + ai * br) * weights).astype(jnp.bfloat16)
        out_ref[j] = folded(gram(re, im, spectra_ref[m]))
        return carry

    lax.fori_loop(0, count, step, 0, unroll=32)


def triad_parts(triads, spectra, weights, groups, mine):
    count = triads.shape[1] // 2
    total, rows, points = spectra.shape
    return pl.pallas_call(
        lambda *refs: triad_kernel(groups, mine, *refs),
        in_specs=[SMEM, VMEM, VMEM],
        out_specs=VMEM,
        out_shape=jax.ShapeDtypeStruct((count, rows // 4, 2 * rows), jnp.float32),
        cost_estimate=pl.CostEstimate(
            flops=count * rows * rows * points * 4,
            bytes_accessed=spectra.size * 2,
            transcendentals=0,
        ),
        compiler_params=params(),
        name="triads_own" if mine else "triads_other",
    )(triads, spectra, weights)


def power_kernel(scale, parts_ref, out_ref):
    total = jnp.sum(parts_ref[...], axis=0) * scale
    half = total.shape[0]
    blocks = 2 * half
    lane = lax.broadcasted_iota(jnp.int32, (1, 4 * blocks), 1)
    lower = lane < 2 * blocks
    other = pltpu.roll(total, 2 * blocks, 1)
    both = jnp.concatenate(
        [jnp.where(lower, total, other), jnp.where(lower, other, total)], axis=0
    )
    sign = jnp.where(lax.rem(lax.div(lane, blocks), 2) == 0, 1.0, -1.0)

    def forward(one, two):
        re = jnp.sum(both * jnp.where(lower, one, 0.0), axis=1, keepdims=True)
        im = jnp.sum(both * jnp.where(lower, two, 0.0), axis=1, keepdims=True)
        return re, im

    def square(one):
        return jnp.sum(jnp.where(lower, one * one, 0.0), axis=1, keepdims=True)

    start = 1.0 / math.sqrt(blocks)
    one = jnp.where(sign > 0, start, 0.0)
    two = jnp.where(sign > 0, 0.0, start)
    for _ in range(ITERS):
        re, im = forward(one, two)
        with_re = jnp.sum(both * re, axis=0, keepdims=True)
        with_im = jnp.sum(both * im, axis=0, keepdims=True)
        one = with_re + sign * pltpu.roll(with_im, blocks, 1)
        two = with_im - sign * pltpu.roll(with_re, blocks, 1)
        factor = 1.0 / jnp.sqrt(square(one) + 1.0)
        one = one * factor
        two = two * factor
    re, im = forward(one, two)
    top = jnp.sum(re * re + im * im, axis=0, keepdims=True)
    energy = top / (blocks * (square(one) + 1.0))
    row = jnp.where(lower, one * sign, energy)
    tail = jnp.broadcast_to(row, (out_ref.shape[1] - half, 4 * blocks))
    for d in range(out_ref.shape[0]):
        out_ref[d, :half] = total
        out_ref[d, half:] = tail


def power(parts, scale, lines):
    _, rows, lanes = parts.shape
    return pl.pallas_call(
        lambda *refs: power_kernel(scale, *refs),
        in_specs=[VMEM],
        out_specs=VMEM,
        out_shape=jax.ShapeDtypeStruct((lines, rows + 8, lanes), jnp.float32),
        compiler_params=params(8),
        name="power",
    )(parts)


def modes_kernel(triads_ref, spectra_ref, vectors_ref, out_ref, pairs_ref):
    total = spectra_ref.shape[0]
    count, lanes = vectors_ref.shape
    blocks = lanes // 4
    lane = lax.broadcasted_iota(jnp.int32, (1, lanes), 1)
    lower = lane < 2 * blocks
    sign = jnp.where(lax.rem(lax.div(lane, blocks), 2) == 0, 1.0, -1.0)
    rows = jnp.where(lower, vectors_ref[...], 0.0)
    rows = rows + pltpu.roll(rows, 2 * blocks, 1)
    swapped = pltpu.roll(rows, blocks, 1)
    odd = lax.rem(lax.broadcasted_iota(jnp.int32, (count, 1), 0), 2) == 1
    keep = lower != odd
    pairs_ref[pl.ds(0, count, stride=2), :] = jnp.where(keep, rows * sign, 0.0)
    pairs_ref[pl.ds(1, count, stride=2), :] = jnp.where(keep, swapped, 0.0)
    early = lax.broadcasted_iota(jnp.int32, (2 * EACH, 1), 0) < EACH

    def step(s, carry):
        picked = []
        for q in range(EACH):
            t = s * EACH + q
            m = lax.rem(triads_ref[0, t] + triads_ref[1, t], total)
            picked.append(spectra_ref[m])
        right = jnp.concatenate(picked, axis=0)
        pair = pairs_ref[pl.ds(pl.multiple_of(s * 2 * EACH, 2 * EACH), 2 * EACH), :]
        left = jnp.concatenate(
            [jnp.where(early, pair, 0.0), jnp.where(early, 0.0, pair)], axis=1
        ).astype(jnp.bfloat16)
        out_ref[s] = jnp.dot(left, right, preferred_element_type=jnp.float32)
        return carry

    lax.fori_loop(0, count // EACH, step, 0, unroll=16)


def modes(triads, spectra, vectors):
    count, lanes = vectors.shape
    total, rows, points = spectra.shape
    return pl.pallas_call(
        modes_kernel,
        in_specs=[SMEM, VMEM, VMEM],
        out_specs=VMEM,
        out_shape=jax.ShapeDtypeStruct((count // EACH, 2 * EACH, points), jnp.float32),
        scratch_shapes=[pltpu.VMEM((2 * count, lanes), jnp.float32)],
        cost_estimate=pl.CostEstimate(
            flops=count * rows * points * 4,
            bytes_accessed=spectra.size * 2,
            transcendentals=0,
        ),
        compiler_params=params(),
        name="modes",
    )(triads, spectra, vectors)


def exchange(value, axis):
    return lax.all_to_all(value, axis, 0, 0, tiled=True)


def swap(value, axis, bit):
    length = lax.axis_size(axis)
    return lax.ppermute(value, axis, [(i, i ^ bit) for i in range(length)])


def unfolded(packed):
    n, half, lanes = packed.shape
    blocks = 2 * half
    parted = packed.reshape(n, half, 2, 2, blocks)
    return parted.transpose(0, 3, 2, 1, 4).reshape(n, 2, blocks, blocks)


def local(spectra, weights, triads):
    groups = lax.axis_size("freq")
    lines = lax.axis_size("line")
    cores = lax.axis_size("core")
    f_dev, _, blocks, points = spectra.shape
    per_group = triads.shape[0] // groups
    point_count = points * lines * cores
    share = points // groups
    weights = weights.reshape(1, points)
    triads = triads.T

    send = cut(spectra.reshape(f_dev * 2 * blocks, points), groups)
    turned = exchange(send, "freq").reshape(groups * f_dev, 2 * blocks, share)

    other = triad_parts(triads, turned, weights, groups, False)
    given = swap(other, "core", 1)
    parts = triad_parts(triads, turned, weights, groups, True) + given
    late_weights, parts = lax.optimization_barrier((weights, parts))
    parts = exchange(parts, ("line", "freq"))

    dens = density_parts(spectra.reshape(f_dev, 2 * blocks, points), late_weights)
    dens = dens + swap(dens, "core", 1)
    for bit in (1, 2, 4):
        dens = dens + swap(dens, "line", bit)
    density = unfolded(dens * (1.0 / point_count))

    payload = power(parts, 1.0 / math.sqrt(blocks * point_count), lines * cores)
    payload = exchange(payload, ("line", "core"))
    bispectrum = unfolded(payload[:, : blocks // 2])
    rows = payload[:, blocks // 2]
    out_vectors = rows[:, : 2 * blocks].reshape(per_group, 2, blocks)
    energy = rows[:, 2 * blocks]

    vectors = exchange(jnp.broadcast_to(rows[None], (groups, *rows.shape)), "freq")
    fields = modes(triads, turned, vectors.reshape(groups * per_group, -1))
    fields = exchange(fields.reshape(groups, 2 * per_group, share), "freq")
    mode_fields = fields.swapaxes(0, 1).reshape(per_group, 2, points)
    return (bispectrum, density, out_vectors, energy, mode_fields)


def solution(mesh):
    pts, freq = mesh.devices.shape
    finer = Mesh(mesh.devices.reshape(pts // 2, 2, freq), ("line", "core", "freq"))
    place = ("line", "core")
    in_specs = (P("freq", None, None, place), P(place), P())
    out_specs = (
        P("freq", None, None, None),
        P("freq", None, None, None),
        P("freq", None, None),
        P("freq"),
        P("freq", None, place),
    )
    return jax.shard_map(local, mesh=finer, in_specs=in_specs, out_specs=out_specs, check_vma=False)
```

```python
import math

import jax
import jax.numpy as jnp
from jax import lax
from jax.experimental import pallas as pl
from jax.experimental.pallas import tpu as pltpu
from jax.sharding import Mesh
from jax.sharding import PartitionSpec as P

ITERS = 3
EACH = 4
NT = (((1,), (1,)), ((), ()))
VMEM = pl.BlockSpec(memory_space=pltpu.VMEM)
SMEM = pl.BlockSpec(memory_space=pltpu.SMEM)


def params(mib=12):
    return pltpu.CompilerParams(vmem_limit_bytes=mib << 20)


def gram(left_re, left_im, right):
    half = right.shape[0] // 2
    right_re, right_im = right[:half], right[half:]
    turned = jnp.concatenate([right_im, -right_re], axis=0)
    return lax.dot_general(
        left_re, right, NT, preferred_element_type=jnp.float32
    ) + lax.dot_general(left_im, turned, NT, preferred_element_type=jnp.float32)


def folded(matrix):
    half = matrix.shape[0] // 2
    return jnp.concatenate([matrix[:half], matrix[half:]], axis=1)


def cut_kernel(rows_ref, out_ref, sems):
    count, _, share = out_ref.shape
    copies = [
        pltpu.make_async_copy(
            rows_ref.at[:, pl.ds(d * share, share)], out_ref.at[d], sems.at[d]
        )
        for d in range(count)
    ]
    for copy in copies:
        copy.start()
    for copy in copies:
        copy.wait()


def cut(rows, count):
    length, points = rows.shape
    return pl.pallas_call(
        cut_kernel,
        in_specs=[pl.BlockSpec(memory_space=pltpu.HBM)],
        out_specs=VMEM,
        out_shape=pltpu.VMEM((count, length, points // count), rows.dtype),
        scratch_shapes=[pltpu.SemaphoreType.DMA((count,))],
        compiler_params=params(),
        name="cut",
    )(pltpu.with_memory_space_constraint(rows, pltpu.HBM))


def density_kernel(spectra_ref, weights_ref, out_ref):
    half = spectra_ref.shape[1] // 2
    for f in range(spectra_ref.shape[0]):
        rows = spectra_ref[f]
        weighted = (rows.astype(jnp.float32) * weights_ref[...]).astype(jnp.bfloat16)
        out_ref[f] = folded(gram(weighted[:half], weighted[half:], rows))


def density_parts(spectra, weights):
    freqs, rows, points = spectra.shape
    return pl.pallas_call(
        density_kernel,
        grid=(freqs // EACH,),
        in_specs=[
            pl.BlockSpec((EACH, rows, points), lambda f: (f, 0, 0)),
            pl.BlockSpec((1, points), lambda f: (0, 0)),
        ],
        out_specs=pl.BlockSpec((EACH, rows // 4, 2 * rows), lambda f: (f, 0, 0)),
        out_shape=jax.ShapeDtypeStruct((freqs, rows // 4, 2 * rows), jnp.float32),
        cost_estimate=pl.CostEstimate(
            flops=freqs * rows * rows * points * 2,
            bytes_accessed=spectra.size * 2,
            transcendentals=0,
        ),
        compiler_params=params(24),
        name="density",
    )(pltpu.with_memory_space_constraint(spectra, pltpu.HBM), weights)


def triad_kernel(groups, mine, triads_ref, spectra_ref, weights_ref, out_ref):
    total, rows, share = spectra_ref.shape
    half = rows // 2
    count = out_ref.shape[0]
    per_group = 2 * count // groups
    core = lax.axis_index("core")
    core = core if mine else 1 - core
    offset = pl.multiple_of(lax.axis_index("freq") * share, share)

    def step(j, carry):
        t = lax.rem(j, groups) * per_group + 2 * lax.div(j, groups) + core
        k = triads_ref[0, t]
        l = triads_ref[1, t]
        m = lax.rem(k + l, total)
        first = spectra_ref[k].astype(jnp.float32)
        second = spectra_ref[l].astype(jnp.float32)
        weights = weights_ref[:, pl.ds(offset, share)]
        ar, ai, br, bi = first[:half], first[half:], second[:half], second[half:]
        re = ((ar * br - ai * bi) * weights).astype(jnp.bfloat16)
        im = ((ar * bi + ai * br) * weights).astype(jnp.bfloat16)
        out_ref[j] = folded(gram(re, im, spectra_ref[m]))
        return carry

    lax.fori_loop(0, count, step, 0, unroll=32)


def triad_parts(triads, spectra, weights, groups, mine):
    count = triads.shape[1] // 2
    total, rows, points = spectra.shape
    return pl.pallas_call(
        lambda *refs: triad_kernel(groups, mine, *refs),
        in_specs=[SMEM, VMEM, VMEM],
        out_specs=VMEM,
        out_shape=jax.ShapeDtypeStruct((count, rows // 4, 2 * rows), jnp.float32),
        cost_estimate=pl.CostEstimate(
            flops=count * rows * rows * points * 4,
            bytes_accessed=spectra.size * 2,
            transcendentals=0,
        ),
        compiler_params=params(),
        name="triads_own" if mine else "triads_other",
    )(triads, spectra, weights)


def power_kernel(scale, parts_ref, out_ref):
    total = jnp.sum(parts_ref[...], axis=0) * scale
    half = total.shape[0]
    blocks = 2 * half
    lane = lax.broadcasted_iota(jnp.int32, (1, 4 * blocks), 1)
    lower = lane < 2 * blocks
    other = pltpu.roll(total, 2 * blocks, 1)
    both = jnp.concatenate(
        [jnp.where(lower, total, other), jnp.where(lower, other, total)], axis=0
    )
    sign = jnp.where(lax.rem(lax.div(lane, blocks), 2) == 0, 1.0, -1.0)

    def forward(one, two):
        re = jnp.sum(both * jnp.where(lower, one, 0.0), axis=1, keepdims=True)
        im = jnp.sum(both * jnp.where(lower, two, 0.0), axis=1, keepdims=True)
        return re, im

    def square(one):
        return jnp.sum(jnp.where(lower, one * one, 0.0), axis=1, keepdims=True)

    start = 1.0 / math.sqrt(blocks)
    one = jnp.where(sign > 0, start, 0.0)
    two = jnp.where(sign > 0, 0.0, start)
    for _ in range(ITERS):
        re, im = forward(one, two)
        with_re = jnp.sum(both * re, axis=0, keepdims=True)
        with_im = jnp.sum(both * im, axis=0, keepdims=True)
        one = with_re + sign * pltpu.roll(with_im, blocks, 1)
        two = with_im - sign * pltpu.roll(with_re, blocks, 1)
        factor = 1.0 / jnp.sqrt(square(one) + 1.0)
        one = one * factor
        two = two * factor
    re, im = forward(one, two)
    top = jnp.sum(re * re + im * im, axis=0, keepdims=True)
    energy = top / (blocks * (square(one) + 1.0))
    row = jnp.where(lower, one * sign, energy)
    tail = jnp.broadcast_to(row, (out_ref.shape[1] - half, 4 * blocks))
    for d in range(out_ref.shape[0]):
        out_ref[d, :half] = total
        out_ref[d, half:] = tail


def power(parts, scale, lines):
    _, rows, lanes = parts.shape
    return pl.pallas_call(
        lambda *refs: power_kernel(scale, *refs),
        in_specs=[VMEM],
        out_specs=VMEM,
        out_shape=jax.ShapeDtypeStruct((lines, rows + 8, lanes), jnp.float32),
        compiler_params=params(8),
        name="power",
    )(parts)


def modes_kernel(triads_ref, spectra_ref, vectors_ref, out_ref, pairs_ref, rows_ref, sems):
    total, height, _ = spectra_ref.shape
    count, lanes = vectors_ref.shape
    blocks = lanes // 4

    def fetch(s, q):
        t = s * EACH + q
        m = lax.rem(triads_ref[0, t] + triads_ref[1, t], total)
        return pltpu.make_async_copy(
            spectra_ref.at[m], rows_ref.at[s, pl.ds(q * height, height)], sems.at[s, q]
        )

    for s in range(count // EACH):
        for q in range(EACH):
            fetch(s, q).start()

    lane = lax.broadcasted_iota(jnp.int32, (1, lanes), 1)
    lower = lane < 2 * blocks
    sign = jnp.where(lax.rem(lax.div(lane, blocks), 2) == 0, 1.0, -1.0)
    rows = jnp.where(lower, vectors_ref[...], 0.0)
    rows = rows + pltpu.roll(rows, 2 * blocks, 1)
    swapped = pltpu.roll(rows, blocks, 1)
    odd = lax.rem(lax.broadcasted_iota(jnp.int32, (count, 1), 0), 2) == 1
    keep = lower != odd
    pairs_ref[pl.ds(0, count, stride=2), :] = jnp.where(keep, rows * sign, 0.0)
    pairs_ref[pl.ds(1, count, stride=2), :] = jnp.where(keep, swapped, 0.0)
    early = lax.broadcasted_iota(jnp.int32, (2 * EACH, 1), 0) < EACH

    for first in range(0, count // EACH, 8):
        for s in range(first, first + 8):
            for q in range(EACH):
                fetch(s, q).wait()
        for s in range(first, first + 8):
            pair = pairs_ref[pl.ds(s * 2 * EACH, 2 * EACH), :]
            left = jnp.concatenate(
                [jnp.where(early, pair, 0.0), jnp.where(early, 0.0, pair)], axis=1
            ).astype(jnp.bfloat16)
            out_ref[s] = jnp.dot(left, rows_ref[s], preferred_element_type=jnp.float32)


def modes(triads, spectra, vectors):
    count, lanes = vectors.shape
    total, rows, points = spectra.shape
    steps = count // EACH
    return pl.pallas_call(
        modes_kernel,
        in_specs=[SMEM, pl.BlockSpec(memory_space=pltpu.HBM), VMEM],
        out_specs=VMEM,
        out_shape=jax.ShapeDtypeStruct((steps, 2 * EACH, points), jnp.float32),
        scratch_shapes=[
            pltpu.VMEM((2 * count, lanes), jnp.float32),
            pltpu.VMEM((steps, EACH * rows, points), spectra.dtype),
            pltpu.SemaphoreType.DMA((steps, EACH)),
        ],
        cost_estimate=pl.CostEstimate(
            flops=count * rows * points * 4,
            bytes_accessed=spectra.size * 2,
            transcendentals=0,
        ),
        compiler_params=params(),
        name="modes",
    )(triads, pltpu.with_memory_space_constraint(spectra, pltpu.HBM), vectors)


def exchange(value, axis):
    return lax.all_to_all(value, axis, 0, 0, tiled=True)


def swap(value, axis, bit):
    length = lax.axis_size(axis)
    return lax.ppermute(value, axis, [(i, i ^ bit) for i in range(length)])


def unfolded(packed):
    n, half, lanes = packed.shape
    blocks = 2 * half
    parted = packed.reshape(n, half, 2, 2, blocks)
    return parted.transpose(0, 3, 2, 1, 4).reshape(n, 2, blocks, blocks)


def local(spectra, weights, triads):
    groups = lax.axis_size("freq")
    lines = lax.axis_size("line")
    cores = lax.axis_size("core")
    f_dev, _, blocks, points = spectra.shape
    per_group = triads.shape[0] // groups
    point_count = points * lines * cores
    share = points // groups
    weights = weights.reshape(1, points)
    triads = triads.T

    send = cut(spectra.reshape(f_dev * 2 * blocks, points), groups)
    turned = exchange(send, "freq").reshape(groups * f_dev, 2 * blocks, share)

    other = triad_parts(triads, turned, weights, groups, False)
    given = swap(other, "core", 1)
    parts = triad_parts(triads, turned, weights, groups, True) + given
    late_weights, parts = lax.optimization_barrier((weights, parts))
    parts = exchange(parts, ("line", "freq"))

    dens = density_parts(spectra.reshape(f_dev, 2 * blocks, points), late_weights)
    dens = dens + swap(dens, "core", 1)

    payload = power(parts, 1.0 / math.sqrt(blocks * point_count), lines * cores)
    payload, dens = lax.optimization_barrier((payload, dens))
    payload = exchange(payload, ("line", "core"))
    dens = dens + swap(dens, "line", 1)

    bispectrum = payload[:, : blocks // 2]
    rows = payload[:, blocks // 2]
    sent = jnp.broadcast_to(rows[None], (groups, *rows.shape))
    sent, dens, bispectrum = lax.optimization_barrier((sent, dens, bispectrum))
    vectors = exchange(sent, "freq")
    dens = dens + swap(dens, "line", 2)

    fields = modes(triads, turned, vectors.reshape(groups * per_group, -1))
    fields, dens, rows = lax.optimization_barrier((fields, dens, rows))
    fields = exchange(fields.reshape(groups, 2 * per_group, share), "freq")
    dens = dens + swap(dens, "line", 4)

    bispectrum = unfolded(bispectrum)
    density = unfolded(dens * (1.0 / point_count))
    out_vectors = rows[:, : 2 * blocks].reshape(per_group, 2, blocks)
    energy = rows[:, 2 * blocks]
    mode_fields = fields.swapaxes(0, 1).reshape(per_group, 2, points)
    return (bispectrum, density, out_vectors, energy, mode_fields)


def solution(mesh):
    pts, freq = mesh.devices.shape
    finer = Mesh(mesh.devices.reshape(pts // 2, 2, freq), ("line", "core", "freq"))
    place = ("line", "core")
    in_specs = (P("freq", None, None, place), P(place), P())
    out_specs = (
        P("freq", None, None, None),
        P("freq", None, None, None),
        P("freq", None, None),
        P("freq"),
        P("freq", None, place),
    )
    return jax.shard_map(local, mesh=finer, in_specs=in_specs, out_specs=out_specs, check_vma=False)
```

```python
import math

import jax
import jax.numpy as jnp
from jax import lax
from jax.experimental import pallas as pl
from jax.experimental.pallas import tpu as pltpu
from jax.sharding import Mesh
from jax.sharding import PartitionSpec as P

ITERS = 3
EACH = 4
NT = (((1,), (1,)), ((), ()))
VMEM = pl.BlockSpec(memory_space=pltpu.VMEM)
SMEM = pl.BlockSpec(memory_space=pltpu.SMEM)


def params(mib=12):
    return pltpu.CompilerParams(vmem_limit_bytes=mib << 20)


def gram(left_re, left_im, right):
    half = right.shape[0] // 2
    right_re, right_im = right[:half], right[half:]
    turned = jnp.concatenate([right_im, -right_re], axis=0)
    return lax.dot_general(
        left_re, right, NT, preferred_element_type=jnp.float32
    ) + lax.dot_general(left_im, turned, NT, preferred_element_type=jnp.float32)


def folded(matrix):
    half = matrix.shape[0] // 2
    return jnp.concatenate([matrix[:half], matrix[half:]], axis=1)


def cut_kernel(rows_ref, out_ref, sems):
    count, _, share = out_ref.shape
    copies = [
        pltpu.make_async_copy(
            rows_ref.at[:, pl.ds(d * share, share)], out_ref.at[d], sems.at[d]
        )
        for d in range(count)
    ]
    for copy in copies:
        copy.start()
    for copy in copies:
        copy.wait()


def cut(rows, count):
    length, points = rows.shape
    return pl.pallas_call(
        cut_kernel,
        in_specs=[pl.BlockSpec(memory_space=pltpu.HBM)],
        out_specs=VMEM,
        out_shape=pltpu.VMEM((count, length, points // count), rows.dtype),
        scratch_shapes=[pltpu.SemaphoreType.DMA((count,))],
        compiler_params=params(),
        name="cut",
    )(pltpu.with_memory_space_constraint(rows, pltpu.HBM))


def sums_kernel(groups, mine, triads_ref, spectra_ref, weights_ref, out_ref):
    total, rows, share = spectra_ref.shape
    half = rows // 2
    fold = half // 2
    count = out_ref.shape[0]
    per_group = 2 * count // groups
    core = lax.axis_index("core")
    core = core if mine else 1 - core
    offset = pl.multiple_of(lax.axis_index("freq") * share, share)

    def step(j, carry):
        t = lax.rem(j, groups) * per_group + 2 * lax.div(j, groups) + core
        k = triads_ref[0, t]
        l = triads_ref[1, t]
        m = lax.rem(k + l, total)
        first = spectra_ref[k].astype(jnp.float32)
        second = spectra_ref[l].astype(jnp.float32)
        weights = weights_ref[:, pl.ds(offset, share)]
        ar, ai, br, bi = first[:half], first[half:], second[:half], second[half:]
        re = ((ar * br - ai * bi) * weights).astype(jnp.bfloat16)
        im = ((ar * bi + ai * br) * weights).astype(jnp.bfloat16)
        out_ref[j, :fold] = folded(gram(re, im, spectra_ref[m]))
        own = spectra_ref[t]
        weighted = (own.astype(jnp.float32) * weights).astype(jnp.bfloat16)
        out_ref[j, fold:] = folded(gram(weighted[:half], weighted[half:], own))
        return carry

    lax.fori_loop(0, count, step, 0, unroll=16)


def sums(triads, spectra, weights, groups, mine):
    count = triads.shape[1] // 2
    total, rows, points = spectra.shape
    return pl.pallas_call(
        lambda *refs: sums_kernel(groups, mine, *refs),
        in_specs=[SMEM, VMEM, VMEM],
        out_specs=VMEM,
        out_shape=jax.ShapeDtypeStruct((count, rows // 2, 2 * rows), jnp.float32),
        cost_estimate=pl.CostEstimate(
            flops=count * rows * rows * points * 8,
            bytes_accessed=spectra.size * 2,
            transcendentals=0,
        ),
        compiler_params=params(),
        name="sums_own" if mine else "sums_other",
    )(triads, spectra, weights)


def pack_kernel(one_ref, two_ref, out_ref):
    fold = one_ref.shape[1] // 2

    def step(j, carry):
        both = one_ref[j] + two_ref[j]
        high = both[:fold].astype(jnp.bfloat16)
        rest = both[:fold] - high.astype(jnp.float32)
        out_ref[j, :fold] = high
        out_ref[j, fold : 2 * fold] = rest.astype(jnp.bfloat16)
        out_ref[j, 2 * fold :] = both[fold:].astype(jnp.bfloat16)
        return carry

    lax.fori_loop(0, one_ref.shape[0], step, 0, unroll=8)


def pack(one, two):
    count, rows, lanes = one.shape
    return pl.pallas_call(
        pack_kernel,
        in_specs=[VMEM, VMEM],
        out_specs=VMEM,
        out_shape=jax.ShapeDtypeStruct((count, 3 * rows // 2, lanes), jnp.bfloat16),
        compiler_params=params(),
        name="pack",
    )(one, two)


def power_kernel(scales, parts_ref, out_ref):
    half = parts_ref.shape[1] // 3
    added = jnp.sum(parts_ref[...].astype(jnp.float32), axis=0)
    total = (added[:half] + added[half : 2 * half]) * scales[0]
    density = added[2 * half :] * scales[1]
    blocks = 2 * half
    lane = lax.broadcasted_iota(jnp.int32, (1, 4 * blocks), 1)
    lower = lane < 2 * blocks
    other = pltpu.roll(total, 2 * blocks, 1)
    both = jnp.concatenate(
        [jnp.where(lower, total, other), jnp.where(lower, other, total)], axis=0
    )
    sign = jnp.where(lax.rem(lax.div(lane, blocks), 2) == 0, 1.0, -1.0)

    def forward(one, two):
        re = jnp.sum(both * jnp.where(lower, one, 0.0), axis=1, keepdims=True)
        im = jnp.sum(both * jnp.where(lower, two, 0.0), axis=1, keepdims=True)
        return re, im

    def square(one):
        return jnp.sum(jnp.where(lower, one * one, 0.0), axis=1, keepdims=True)

    start = 1.0 / math.sqrt(blocks)
    one = jnp.where(sign > 0, start, 0.0)
    two = jnp.where(sign > 0, 0.0, start)
    for _ in range(ITERS):
        re, im = forward(one, two)
        with_re = jnp.sum(both * re, axis=0, keepdims=True)
        with_im = jnp.sum(both * im, axis=0, keepdims=True)
        one = with_re + sign * pltpu.roll(with_im, blocks, 1)
        two = with_im - sign * pltpu.roll(with_re, blocks, 1)
        factor = 1.0 / jnp.sqrt(square(one) + 1.0)
        one = one * factor
        two = two * factor
    re, im = forward(one, two)
    top = jnp.sum(re * re + im * im, axis=0, keepdims=True)
    energy = top / (blocks * (square(one) + 1.0))
    row = jnp.where(lower, one * sign, energy)
    tail = jnp.broadcast_to(row, (out_ref.shape[1] - 2 * half, 4 * blocks))
    for d in range(out_ref.shape[0]):
        out_ref[d, :half] = total
        out_ref[d, half : 2 * half] = density
        out_ref[d, 2 * half :] = tail


def power(parts, scales, lines):
    _, rows, lanes = parts.shape
    return pl.pallas_call(
        lambda *refs: power_kernel(scales, *refs),
        in_specs=[VMEM],
        out_specs=VMEM,
        out_shape=jax.ShapeDtypeStruct((lines, 2 * rows // 3 + 8, lanes), jnp.float32),
        compiler_params=params(8),
        name="power",
    )(parts)


def modes_kernel(triads_ref, spectra_ref, vectors_ref, out_ref, pairs_ref):
    total = spectra_ref.shape[0]
    count, lanes = vectors_ref.shape
    blocks = lanes // 4
    lane = lax.broadcasted_iota(jnp.int32, (1, lanes), 1)
    lower = lane < 2 * blocks
    sign = jnp.where(lax.rem(lax.div(lane, blocks), 2) == 0, 1.0, -1.0)
    rows = jnp.where(lower, vectors_ref[...], 0.0)
    rows = rows + pltpu.roll(rows, 2 * blocks, 1)
    swapped = pltpu.roll(rows, blocks, 1)
    odd = lax.rem(lax.broadcasted_iota(jnp.int32, (count, 1), 0), 2) == 1
    keep = lower != odd
    pairs_ref[pl.ds(0, count, stride=2), :] = jnp.where(keep, rows * sign, 0.0)
    pairs_ref[pl.ds(1, count, stride=2), :] = jnp.where(keep, swapped, 0.0)
    early = lax.broadcasted_iota(jnp.int32, (2 * EACH, 1), 0) < EACH

    def step(s, carry):
        picked = []
        for q in range(EACH):
            t = s * EACH + q
            m = lax.rem(triads_ref[0, t] + triads_ref[1, t], total)
            picked.append(spectra_ref[m])
        right = jnp.concatenate(picked, axis=0)
        pair = pairs_ref[pl.ds(pl.multiple_of(s * 2 * EACH, 2 * EACH), 2 * EACH), :]
        left = jnp.concatenate(
            [jnp.where(early, pair, 0.0), jnp.where(early, 0.0, pair)], axis=1
        ).astype(jnp.bfloat16)
        out_ref[s] = jnp.dot(left, right, preferred_element_type=jnp.float32)
        return carry

    lax.fori_loop(0, count // EACH, step, 0, unroll=16)


def modes(triads, spectra, vectors):
    count, lanes = vectors.shape
    total, rows, points = spectra.shape
    return pl.pallas_call(
        modes_kernel,
        in_specs=[SMEM, VMEM, VMEM],
        out_specs=VMEM,
        out_shape=jax.ShapeDtypeStruct((count // EACH, 2 * EACH, points), jnp.float32),
        scratch_shapes=[pltpu.VMEM((2 * count, lanes), jnp.float32)],
        cost_estimate=pl.CostEstimate(
            flops=count * rows * points * 4,
            bytes_accessed=spectra.size * 2,
            transcendentals=0,
        ),
        compiler_params=params(),
        name="modes",
    )(triads, spectra, vectors)


def exchange(value, axis):
    return lax.all_to_all(value, axis, 0, 0, tiled=True)


def swap(value, axis, bit):
    length = lax.axis_size(axis)
    return lax.ppermute(value, axis, [(i, i ^ bit) for i in range(length)])


def unfolded(packed):
    n, half, lanes = packed.shape
    blocks = 2 * half
    parted = packed.reshape(n, half, 2, 2, blocks)
    return parted.transpose(0, 3, 2, 1, 4).reshape(n, 2, blocks, blocks)


def local(spectra, weights, triads):
    groups = lax.axis_size("freq")
    lines = lax.axis_size("line")
    cores = lax.axis_size("core")
    f_dev, _, blocks, points = spectra.shape
    per_group = triads.shape[0] // groups
    point_count = points * lines * cores
    share = points // groups
    weights = weights.reshape(1, points)
    triads = triads.T

    send = cut(spectra.reshape(f_dev * 2 * blocks, points), groups)
    turned = exchange(send, "freq").reshape(groups * f_dev, 2 * blocks, share)

    other = sums(triads, turned, weights, groups, False)
    given = swap(other, "core", 1)
    parts = pack(sums(triads, turned, weights, groups, True), given)
    parts = exchange(parts, ("line", "freq"))

    scales = (1.0 / math.sqrt(blocks * point_count), 1.0 / point_count)
    payload = power(parts, scales, lines * cores)
    payload = exchange(payload, ("line", "core"))
    fold = blocks // 2
    rows = payload[:, 2 * fold]
    vectors = exchange(jnp.broadcast_to(rows[None], (groups, *rows.shape)), "freq")
    fields = modes(triads, turned, vectors.reshape(groups * per_group, -1))
    fields = exchange(fields.reshape(groups, 2 * per_group, share), "freq")

    bispectrum = unfolded(payload[:, :fold])
    density = unfolded(payload[:, fold : 2 * fold])
    out_vectors = rows[:, : 2 * blocks].reshape(per_group, 2, blocks)
    energy = rows[:, 2 * blocks]
    mode_fields = fields.swapaxes(0, 1).reshape(per_group, 2, points)
    return (bispectrum, density, out_vectors, energy, mode_fields)


def solution(mesh):
    pts, freq = mesh.devices.shape
    finer = Mesh(mesh.devices.reshape(pts // 2, 2, freq), ("line", "core", "freq"))
    place = ("line", "core")
    in_specs = (P("freq", None, None, place), P(place), P())
    out_specs = (
        P("freq", None, None, None),
        P("freq", None, None, None),
        P("freq", None, None),
        P("freq"),
        P("freq", None, place),
    )
    return jax.shard_map(local, mesh=finer, in_specs=in_specs, out_specs=out_specs, check_vma=False)
```

```python
import math

import jax
import jax.numpy as jnp
from jax import lax
from jax.experimental import pallas as pl
from jax.experimental.pallas import tpu as pltpu
from jax.sharding import Mesh
from jax.sharding import PartitionSpec as P

ITERS = 3
EACH = 4
NT = (((1,), (1,)), ((), ()))
VMEM = pl.BlockSpec(memory_space=pltpu.VMEM)
SMEM = pl.BlockSpec(memory_space=pltpu.SMEM)


def params(mib=12):
    return pltpu.CompilerParams(vmem_limit_bytes=mib << 20)


def gram(left, right):
    half = right.shape[0] // 2
    joined = lax.dot_general(left, right, NT, preferred_element_type=jnp.float32)
    upper, lower = joined[:half], joined[half:]
    return upper + jnp.concatenate([lower[:, half:], -lower[:, :half]], axis=1)


def folded(matrix):
    half = matrix.shape[0] // 2
    return jnp.concatenate([matrix[:half], matrix[half:]], axis=1)


def cut_kernel(rows_ref, out_ref, sems):
    count, _, share = out_ref.shape
    copies = [
        pltpu.make_async_copy(
            rows_ref.at[:, pl.ds(d * share, share)], out_ref.at[d], sems.at[d]
        )
        for d in range(count)
    ]
    for copy in copies:
        copy.start()
    for copy in copies:
        copy.wait()


def cut(rows, count):
    length, points = rows.shape
    return pl.pallas_call(
        cut_kernel,
        in_specs=[pl.BlockSpec(memory_space=pltpu.HBM)],
        out_specs=VMEM,
        out_shape=pltpu.VMEM((count, length, points // count), rows.dtype),
        scratch_shapes=[pltpu.SemaphoreType.DMA((count,))],
        compiler_params=params(),
        name="cut",
    )(pltpu.with_memory_space_constraint(rows, pltpu.HBM))


def sums_kernel(groups, mine, triads_ref, spectra_ref, weights_ref, out_ref):
    total, rows, share = spectra_ref.shape
    half = rows // 2
    fold = half // 2
    count = out_ref.shape[0]
    per_group = 2 * count // groups
    core = lax.axis_index("core")
    core = core if mine else 1 - core
    offset = pl.multiple_of(lax.axis_index("freq") * share, share)

    def step(j, carry):
        t = lax.rem(j, groups) * per_group + 2 * lax.div(j, groups) + core
        k = triads_ref[0, t]
        l = triads_ref[1, t]
        m = lax.rem(k + l, total)
        first = spectra_ref[k].astype(jnp.float32)
        second = spectra_ref[l].astype(jnp.float32)
        weights = weights_ref[:, pl.ds(offset, share)]
        ar, ai, br, bi = first[:half], first[half:], second[:half], second[half:]
        re = ((ar * br - ai * bi) * weights).astype(jnp.bfloat16)
        im = ((ar * bi + ai * br) * weights).astype(jnp.bfloat16)
        product = jnp.concatenate([re, im], axis=0)
        out_ref[j, :fold] = folded(gram(product, spectra_ref[m]))
        own = spectra_ref[t]
        weighted = (own.astype(jnp.float32) * weights).astype(jnp.bfloat16)
        out_ref[j, fold:] = folded(gram(weighted, own))
        return carry

    lax.fori_loop(0, count, step, 0, unroll=32)


def sums(triads, spectra, weights, groups, mine):
    count = triads.shape[1] // 2
    total, rows, points = spectra.shape
    return pl.pallas_call(
        lambda *refs: sums_kernel(groups, mine, *refs),
        in_specs=[SMEM, VMEM, VMEM],
        out_specs=VMEM,
        out_shape=jax.ShapeDtypeStruct((count, rows // 2, 2 * rows), jnp.float32),
        cost_estimate=pl.CostEstimate(
            flops=count * rows * rows * points * 8,
            bytes_accessed=spectra.size * 2,
            transcendentals=0,
        ),
        compiler_params=params(),
        name="sums_own" if mine else "sums_other",
    )(triads, spectra, weights)


def pack_kernel(one_ref, two_ref, out_ref):
    fold = one_ref.shape[1] // 2

    def step(j, carry):
        both = one_ref[j] + two_ref[j]
        high = both[:fold].astype(jnp.bfloat16)
        rest = both[:fold] - high.astype(jnp.float32)
        out_ref[j, :fold] = high
        out_ref[j, fold : 2 * fold] = rest.astype(jnp.bfloat16)
        out_ref[j, 2 * fold :] = both[fold:].astype(jnp.bfloat16)
        return carry

    lax.fori_loop(0, one_ref.shape[0], step, 0, unroll=8)


def pack(one, two):
    count, rows, lanes = one.shape
    return pl.pallas_call(
        pack_kernel,
        in_specs=[VMEM, VMEM],
        out_specs=VMEM,
        out_shape=jax.ShapeDtypeStruct((count, 3 * rows // 2, lanes), jnp.bfloat16),
        compiler_params=params(),
        name="pack",
    )(one, two)


def power_kernel(scales, parts_ref, out_ref):
    half = parts_ref.shape[1] // 3
    added = jnp.sum(parts_ref[...].astype(jnp.float32), axis=0)
    total = (added[:half] + added[half : 2 * half]) * scales[0]
    density = added[2 * half :] * scales[1]
    blocks = 2 * half
    lane = lax.broadcasted_iota(jnp.int32, (1, 4 * blocks), 1)
    lower = lane < 2 * blocks
    other = pltpu.roll(total, 2 * blocks, 1)
    both = jnp.concatenate(
        [jnp.where(lower, total, other), jnp.where(lower, other, total)], axis=0
    )
    sign = jnp.where(lax.rem(lax.div(lane, blocks), 2) == 0, 1.0, -1.0)

    def forward(one, two):
        re = jnp.sum(both * jnp.where(lower, one, 0.0), axis=1, keepdims=True)
        im = jnp.sum(both * jnp.where(lower, two, 0.0), axis=1, keepdims=True)
        return re, im

    def square(one):
        return jnp.sum(jnp.where(lower, one * one, 0.0), axis=1, keepdims=True)

    start = 1.0 / math.sqrt(blocks)
    one = jnp.where(sign > 0, start, 0.0)
    two = jnp.where(sign > 0, 0.0, start)
    for _ in range(ITERS):
        re, im = forward(one, two)
        with_re = jnp.sum(both * re, axis=0, keepdims=True)
        with_im = jnp.sum(both * im, axis=0, keepdims=True)
        one = with_re + sign * pltpu.roll(with_im, blocks, 1)
        two = with_im - sign * pltpu.roll(with_re, blocks, 1)
        factor = 1.0 / jnp.sqrt(square(one) + 1.0)
        one = one * factor
        two = two * factor
    re, im = forward(one, two)
    top = jnp.sum(re * re + im * im, axis=0, keepdims=True)
    energy = top / (blocks * (square(one) + 1.0))
    row = jnp.where(lower, one * sign, energy)
    tail = jnp.broadcast_to(row, (out_ref.shape[1] - 2 * half, 4 * blocks))
    for d in range(out_ref.shape[0]):
        out_ref[d, :half] = total
        out_ref[d, half : 2 * half] = density
        out_ref[d, 2 * half :] = tail


def power(parts, scales, lines):
    _, rows, lanes = parts.shape
    return pl.pallas_call(
        lambda *refs: power_kernel(scales, *refs),
        in_specs=[VMEM],
        out_specs=VMEM,
        out_shape=jax.ShapeDtypeStruct((lines, 2 * rows // 3 + 8, lanes), jnp.float32),
        compiler_params=params(8),
        name="power",
    )(parts)


def modes_kernel(triads_ref, spectra_ref, vectors_ref, out_ref, pairs_ref):
    total = spectra_ref.shape[0]
    count, lanes = vectors_ref.shape
    blocks = lanes // 4
    lane = lax.broadcasted_iota(jnp.int32, (1, lanes), 1)
    lower = lane < 2 * blocks
    sign = jnp.where(lax.rem(lax.div(lane, blocks), 2) == 0, 1.0, -1.0)
    rows = jnp.where(lower, vectors_ref[...], 0.0)
    rows = rows + pltpu.roll(rows, 2 * blocks, 1)
    swapped = pltpu.roll(rows, blocks, 1)
    odd = lax.rem(lax.broadcasted_iota(jnp.int32, (count, 1), 0), 2) == 1
    keep = lower != odd
    pairs_ref[pl.ds(0, count, stride=2), :] = jnp.where(keep, rows * sign, 0.0)
    pairs_ref[pl.ds(1, count, stride=2), :] = jnp.where(keep, swapped, 0.0)
    early = lax.broadcasted_iota(jnp.int32, (2 * EACH, 1), 0) < EACH

    def step(s, carry):
        picked = []
        for q in range(EACH):
            t = s * EACH + q
            m = lax.rem(triads_ref[0, t] + triads_ref[1, t], total)
            picked.append(spectra_ref[m])
        right = jnp.concatenate(picked, axis=0)
        pair = pairs_ref[pl.ds(pl.multiple_of(s * 2 * EACH, 2 * EACH), 2 * EACH), :]
        left = jnp.concatenate(
            [jnp.where(early, pair, 0.0), jnp.where(early, 0.0, pair)], axis=1
        ).astype(jnp.bfloat16)
        mixed = jnp.dot(left, right, preferred_element_type=jnp.float32)
        out_ref[s] = mixed.astype(out_ref.dtype)
        return carry

    lax.fori_loop(0, count // EACH, step, 0, unroll=16)


def modes(triads, spectra, vectors):
    count, lanes = vectors.shape
    total, rows, points = spectra.shape
    return pl.pallas_call(
        modes_kernel,
        in_specs=[SMEM, VMEM, VMEM],
        out_specs=VMEM,
        out_shape=jax.ShapeDtypeStruct((count // EACH, 2 * EACH, points), jnp.bfloat16),
        scratch_shapes=[pltpu.VMEM((2 * count, lanes), jnp.float32)],
        cost_estimate=pl.CostEstimate(
            flops=count * rows * points * 4,
            bytes_accessed=spectra.size * 2,
            transcendentals=0,
        ),
        compiler_params=params(),
        name="modes",
    )(triads, spectra, vectors)


def spread_kernel(payload_ref, out_ref):
    rows = payload_ref[:, payload_ref.shape[1] - 1]
    for d in range(out_ref.shape[0]):
        out_ref[d] = rows


def spread(payload, groups):
    count, _, lanes = payload.shape
    return pl.pallas_call(
        spread_kernel,
        in_specs=[VMEM],
        out_specs=VMEM,
        out_shape=jax.ShapeDtypeStruct((groups, count, lanes), jnp.float32),
        compiler_params=params(8),
        name="spread",
    )(payload)


def finish_kernel(fields_ref, payload_ref, bis_ref, dens_ref, vec_ref, energy_ref, modes_ref):
    count, _, lanes = payload_ref.shape
    blocks = lanes // 4
    fold = blocks // 2
    share = fields_ref.shape[2]
    for t in range(count):
        for first, to_ref in ((0, bis_ref), (fold, dens_ref)):
            packed = payload_ref[t, first : first + fold]
            for part in range(4):
                low, ri = part // 2, part % 2
                piece = packed[:, part * blocks : (part + 1) * blocks]
                to_ref[t, ri, low * fold : (low + 1) * fold, :] = piece
    rows = payload_ref[:, payload_ref.shape[1] - 1]
    for t in range(count):
        for ri in range(2):
            vec_ref[t, ri : ri + 1, :] = rows[t : t + 1, ri * blocks : (ri + 1) * blocks]
    lane = lax.broadcasted_iota(jnp.int32, rows.shape, 1)
    index = lax.broadcasted_iota(jnp.int32, rows.shape, 0)
    own = jnp.where(lane == index + 2 * blocks, rows, 0.0)
    line = pltpu.roll(jnp.sum(own, axis=0, keepdims=True), 2 * blocks, 1)
    energy_ref[...] = line[:, :count]
    for g in range(fields_ref.shape[0]):
        block = fields_ref[g].astype(jnp.float32)
        for t in range(count):
            modes_ref[t, :, g * share : (g + 1) * share] = block[2 * t : 2 * t + 2]


def finish(fields, payload):
    count, _, lanes = payload.shape
    groups, _, share = fields.shape
    blocks = lanes // 4
    square = jax.ShapeDtypeStruct((count, 2, blocks, blocks), jnp.float32)
    bispectrum, density, vectors, energy, mode_fields = pl.pallas_call(
        finish_kernel,
        in_specs=[VMEM, VMEM],
        out_specs=[VMEM] * 5,
        out_shape=[
            square,
            square,
            jax.ShapeDtypeStruct((count, 2, blocks), jnp.float32),
            jax.ShapeDtypeStruct((1, count), jnp.float32),
            jax.ShapeDtypeStruct((count, 2, groups * share), jnp.float32),
        ],
        compiler_params=params(8),
        name="finish",
    )(fields, payload)
    return (bispectrum, density, vectors, energy.reshape(count), mode_fields)


def exchange(value, axis):
    return lax.all_to_all(value, axis, 0, 0, tiled=True)


def swap(value, axis, bit):
    length = lax.axis_size(axis)
    return lax.ppermute(value, axis, [(i, i ^ bit) for i in range(length)])


def local(spectra, weights, triads):
    groups = lax.axis_size("freq")
    lines = lax.axis_size("line")
    cores = lax.axis_size("core")
    f_dev, _, blocks, points = spectra.shape
    per_group = triads.shape[0] // groups
    point_count = points * lines * cores
    share = points // groups
    weights = weights.reshape(1, points)
    triads = triads.T

    send = cut(spectra.reshape(f_dev * 2 * blocks, points), groups)
    turned = exchange(send, "freq").reshape(groups * f_dev, 2 * blocks, share)

    other = sums(triads, turned, weights, groups, False)
    given = swap(other, "core", 1)
    parts = pack(sums(triads, turned, weights, groups, True), given)
    parts = exchange(parts, ("line", "freq"))

    scales = (1.0 / math.sqrt(blocks * point_count), 1.0 / point_count)
    payload = power(parts, scales, lines * cores)
    payload = exchange(payload, ("line", "core"))
    vectors = exchange(spread(payload, groups), "freq")
    fields = modes(triads, turned, vectors.reshape(groups * per_group, -1))
    fields = exchange(fields.reshape(groups, 2 * per_group, share), "freq")
    return finish(fields, payload)


def solution(mesh):
    pts, freq = mesh.devices.shape
    finer = Mesh(mesh.devices.reshape(pts // 2, 2, freq), ("line", "core", "freq"))
    place = ("line", "core")
    in_specs = (P("freq", None, None, place), P(place), P())
    out_specs = (
        P("freq", None, None, None),
        P("freq", None, None, None),
        P("freq", None, None),
        P("freq"),
        P("freq", None, place),
    )
    return jax.shard_map(local, mesh=finer, in_specs=in_specs, out_specs=out_specs, check_vma=False)
```

```python
import math

import jax
import jax.numpy as jnp
from jax import lax
from jax.experimental import pallas as pl
from jax.experimental.pallas import tpu as pltpu
from jax.sharding import Mesh
from jax.sharding import PartitionSpec as P

ITERS = 3
EACH = 4
NT = (((1,), (1,)), ((), ()))
VMEM = pl.BlockSpec(memory_space=pltpu.VMEM)
SMEM = pl.BlockSpec(memory_space=pltpu.SMEM)


def params(mib=12):
    return pltpu.CompilerParams(vmem_limit_bytes=mib << 20)


def gram(left, right):
    half = right.shape[0] // 2
    joined = lax.dot_general(left, right, NT, preferred_element_type=jnp.float32)
    upper, lower = joined[:half], joined[half:]
    return upper + jnp.concatenate([lower[:, half:], -lower[:, :half]], axis=1)


def folded(matrix):
    half = matrix.shape[0] // 2
    return jnp.concatenate([matrix[:half], matrix[half:]], axis=1)


def cut_kernel(rows_ref, out_ref, sems):
    count, _, share = out_ref.shape
    copies = [
        pltpu.make_async_copy(
            rows_ref.at[:, pl.ds(d * share, share)], out_ref.at[d], sems.at[d]
        )
        for d in range(count)
    ]
    for copy in copies:
        copy.start()
    for copy in copies:
        copy.wait()


def cut(rows, count):
    length, points = rows.shape
    return pl.pallas_call(
        cut_kernel,
        in_specs=[pl.BlockSpec(memory_space=pltpu.HBM)],
        out_specs=VMEM,
        out_shape=pltpu.VMEM((count, length, points // count), rows.dtype),
        scratch_shapes=[pltpu.SemaphoreType.DMA((count,))],
        compiler_params=params(),
        name="cut",
    )(pltpu.with_memory_space_constraint(rows, pltpu.HBM))


def sums_kernel(groups, mine, triads_ref, spectra_ref, weights_ref, out_ref):
    total, rows, share = spectra_ref.shape
    half = rows // 2
    fold = half // 2
    count = out_ref.shape[0]
    per_group = 2 * count // groups
    core = lax.axis_index("core")
    core = core if mine else 1 - core
    offset = pl.multiple_of(lax.axis_index("freq") * share, share)

    def step(j, carry):
        t = lax.rem(j, groups) * per_group + 2 * lax.div(j, groups) + core
        k = triads_ref[0, t]
        l = triads_ref[1, t]
        m = lax.rem(k + l, total)
        first = spectra_ref[k].astype(jnp.float32)
        second = spectra_ref[l].astype(jnp.float32)
        weights = weights_ref[:, pl.ds(offset, share)]
        ar, ai, br, bi = first[:half], first[half:], second[:half], second[half:]
        re = ((ar * br - ai * bi) * weights).astype(jnp.bfloat16)
        im = ((ar * bi + ai * br) * weights).astype(jnp.bfloat16)
        product = jnp.concatenate([re, im], axis=0)
        out_ref[j, :fold] = folded(gram(product, spectra_ref[m]))
        own = spectra_ref[t]
        weighted = (own.astype(jnp.float32) * weights).astype(jnp.bfloat16)
        out_ref[j, fold:] = folded(gram(weighted, own))
        return carry

    lax.fori_loop(0, count, step, 0, unroll=32)


def sums(triads, spectra, weights, groups, mine):
    count = triads.shape[1] // 2
    total, rows, points = spectra.shape
    return pl.pallas_call(
        lambda *refs: sums_kernel(groups, mine, *refs),
        in_specs=[SMEM, VMEM, VMEM],
        out_specs=VMEM,
        out_shape=jax.ShapeDtypeStruct((count, rows // 2, 2 * rows), jnp.float32),
        cost_estimate=pl.CostEstimate(
            flops=count * rows * rows * points * 8,
            bytes_accessed=spectra.size * 2,
            transcendentals=0,
        ),
        compiler_params=params(),
        name="sums_own" if mine else "sums_other",
    )(triads, spectra, weights)


def pack_kernel(one_ref, two_ref, out_ref):
    fold = one_ref.shape[1] // 2

    def step(j, carry):
        both = one_ref[j] + two_ref[j]
        high = both[:fold].astype(jnp.bfloat16)
        rest = both[:fold] - high.astype(jnp.float32)
        out_ref[j, :fold] = high
        out_ref[j, fold : 2 * fold] = rest.astype(jnp.bfloat16)
        out_ref[j, 2 * fold :] = both[fold:].astype(jnp.bfloat16)
        return carry

    lax.fori_loop(0, one_ref.shape[0], step, 0, unroll=8)


def pack(one, two):
    count, rows, lanes = one.shape
    return pl.pallas_call(
        pack_kernel,
        in_specs=[VMEM, VMEM],
        out_specs=VMEM,
        out_shape=jax.ShapeDtypeStruct((count, 3 * rows // 2, lanes), jnp.bfloat16),
        compiler_params=params(),
        name="pack",
    )(one, two)


def high_of(value):
    return value.astype(jnp.bfloat16).astype(jnp.float32)


def power_kernel(scales, groups, parts_ref, out_ref, held_ref):
    half = parts_ref.shape[1] // 3
    added = jnp.sum(parts_ref[...].astype(jnp.float32), axis=0)
    total = (added[:half] + added[half : 2 * half]) * scales[0]
    density = added[2 * half :] * scales[1]
    blocks = 2 * half
    lane = lax.broadcasted_iota(jnp.int32, (1, 4 * blocks), 1)
    lower = lane < 2 * blocks
    other = pltpu.roll(total, 2 * blocks, 1)
    both = jnp.concatenate(
        [jnp.where(lower, total, other), jnp.where(lower, other, total)], axis=0
    )
    sign = jnp.where(lax.rem(lax.div(lane, blocks), 2) == 0, 1.0, -1.0)

    def forward(one, two):
        re = jnp.sum(both * jnp.where(lower, one, 0.0), axis=1, keepdims=True)
        im = jnp.sum(both * jnp.where(lower, two, 0.0), axis=1, keepdims=True)
        return re, im

    def square(one):
        return jnp.sum(jnp.where(lower, one * one, 0.0), axis=1, keepdims=True)

    start = 1.0 / math.sqrt(blocks)
    one = jnp.where(sign > 0, start, 0.0)
    two = jnp.where(sign > 0, 0.0, start)
    for _ in range(ITERS):
        re, im = forward(one, two)
        with_re = jnp.sum(both * re, axis=0, keepdims=True)
        with_im = jnp.sum(both * im, axis=0, keepdims=True)
        one = with_re + sign * pltpu.roll(with_im, blocks, 1)
        two = with_im - sign * pltpu.roll(with_re, blocks, 1)
        factor = 1.0 / jnp.sqrt(square(one) + 1.0)
        one = one * factor
        two = two * factor
    re, im = forward(one, two)
    top = jnp.sum(re * re + im * im, axis=0, keepdims=True)
    energy = top / (blocks * (square(one) + 1.0))
    row = jnp.where(lower, one * sign, energy)
    row_high, total_high = high_of(row), high_of(total)
    row_rest, total_rest = row - row_high, total - total_high
    for g in range(groups):
        held_ref[8 * g : 8 * g + 1] = row_high
        held_ref[8 * g + 1 : 8 * g + 2] = row_rest
        held_ref[8 * g + 2 : 8 * g + 4] = total_high[2 * g : 2 * g + 2]
        held_ref[8 * g + 4 : 8 * g + 6] = total_rest[2 * g : 2 * g + 2]
        held_ref[8 * g + 6 : 8 * g + 8] = density[2 * g : 2 * g + 2]
    slices = [held_ref[8 * g : 8 * g + 8].astype(out_ref.dtype) for g in range(groups)]
    for d in range(out_ref.shape[0]):
        out_ref[d] = slices[d % groups]


def power(parts, scales, groups, count):
    _, rows, lanes = parts.shape
    assert rows == 6 * groups
    return pl.pallas_call(
        lambda *refs: power_kernel(scales, groups, *refs),
        in_specs=[VMEM],
        out_specs=VMEM,
        out_shape=jax.ShapeDtypeStruct((count, 8, lanes), jnp.bfloat16),
        scratch_shapes=[pltpu.VMEM((8 * groups, lanes), jnp.float32)],
        compiler_params=params(8),
        name="power",
    )(parts)


def modes_kernel(triads_ref, spectra_ref, slices_ref, out_ref, pairs_ref, wide_ref, vectors_ref):
    total = spectra_ref.shape[0]
    count, height, lanes = slices_ref.shape
    groups = out_ref.shape[0]
    per_group = count // groups
    blocks = lanes // 4
    wide_ref[...] = slices_ref[...].astype(jnp.float32).reshape(count * height, lanes)
    for g in range(groups):
        vectors_ref[g * per_group : (g + 1) * per_group] = wide_ref[
            pl.ds(g * height, per_group, stride=groups * height), :
        ]
    lane = lax.broadcasted_iota(jnp.int32, (1, lanes), 1)
    lower = lane < 2 * blocks
    sign = jnp.where(lax.rem(lax.div(lane, blocks), 2) == 0, 1.0, -1.0)
    rows = jnp.where(lower, vectors_ref[...], 0.0)
    rows = rows + pltpu.roll(rows, 2 * blocks, 1)
    swapped = pltpu.roll(rows, blocks, 1)
    odd = lax.rem(lax.broadcasted_iota(jnp.int32, (count, 1), 0), 2) == 1
    keep = lower != odd
    pairs_ref[pl.ds(0, count, stride=2), :] = jnp.where(keep, rows * sign, 0.0)
    pairs_ref[pl.ds(1, count, stride=2), :] = jnp.where(keep, swapped, 0.0)
    early = lax.broadcasted_iota(jnp.int32, (2 * EACH, 1), 0) < EACH
    steps = per_group // EACH
    after = 2 * steps * 2 * EACH
    for g in range(groups):
        for s in range(steps):
            picked = []
            for q in range(EACH):
                t = g * per_group + s * EACH + q
                m = lax.rem(triads_ref[0, t] + triads_ref[1, t], total)
                picked.append(spectra_ref[m])
            right = jnp.concatenate(picked, axis=0)
            pair = pairs_ref[pl.ds(2 * (g * per_group + s * EACH), 2 * EACH), :]
            left = jnp.concatenate(
                [jnp.where(early, pair, 0.0), jnp.where(early, 0.0, pair)], axis=1
            ).astype(jnp.bfloat16)
            mixed = jnp.dot(left, right, preferred_element_type=jnp.float32)
            mixed = mixed.astype(out_ref.dtype)
            for h in range(2):
                at = (h * steps + s) * 2 * EACH
                out_ref[g, at : at + 2 * EACH] = mixed[:, h * lanes : (h + 1) * lanes]
        for i in range(per_group):
            at = after + height * i
            out_ref[g, at : at + height] = slices_ref[i * groups + g]


def modes(triads, spectra, slices, groups):
    count, height, lanes = slices.shape
    total, rows, points = spectra.shape
    assert points == 2 * lanes
    per_group = count // groups
    return pl.pallas_call(
        modes_kernel,
        in_specs=[SMEM, VMEM, VMEM],
        out_specs=VMEM,
        out_shape=jax.ShapeDtypeStruct((groups, (4 + height) * per_group, lanes), jnp.bfloat16),
        scratch_shapes=[
            pltpu.VMEM((2 * count, lanes), jnp.float32),
            pltpu.VMEM((count * height, lanes), jnp.float32),
            pltpu.VMEM((count, lanes), jnp.float32),
        ],
        cost_estimate=pl.CostEstimate(
            flops=count * rows * points * 4,
            bytes_accessed=spectra.size * 2,
            transcendentals=0,
        ),
        compiler_params=params(),
        name="modes",
    )(triads, spectra, slices)


def finish_kernel(got_ref, bis_ref, dens_ref, vec_ref, energy_ref, modes_ref, wide_ref):
    groups, _, lanes = got_ref.shape
    count = modes_ref.shape[0]
    blocks = lanes // 4
    fold = blocks // 2
    first = 4 * count

    def spread(value, row, to_ref):
        for part in range(4):
            low, ri = part // 2, part % 2
            at = ri * blocks + low * fold + row
            piece = value[:, part * blocks : (part + 1) * blocks]
            to_ref[pl.ds(at, count, stride=2 * blocks), :] = piece

    for g in range(groups):
        wide_ref[...] = got_ref[g, first:].astype(jnp.float32)

        def every(k):
            return wide_ref[pl.ds(k, count, stride=8), :]

        for r in range(2):
            spread(every(2 + r) + every(4 + r), 2 * g + r, bis_ref)
            spread(every(6 + r), 2 * g + r, dens_ref)
        if g == 0:
            rows = every(0) + every(1)
            for t in range(count):
                for ri in range(2):
                    part = rows[t : t + 1, ri * blocks : (ri + 1) * blocks]
                    vec_ref[t, ri : ri + 1, :] = part
            lane = lax.broadcasted_iota(jnp.int32, rows.shape, 1)
            index = lax.broadcasted_iota(jnp.int32, rows.shape, 0)
            own = jnp.where(lane == index + 2 * blocks, rows, 0.0)
            line = pltpu.roll(jnp.sum(own, axis=0, keepdims=True), 2 * blocks, 1)
            energy_ref[...] = line[:, :count]
        for h in range(2):
            block = got_ref[g, h * 2 * count : (h + 1) * 2 * count].astype(jnp.float32)
            at = (2 * g + h) * lanes
            for t in range(count):
                modes_ref[t, :, at : at + lanes] = block[2 * t : 2 * t + 2]


def finish(got):
    groups, rows, lanes = got.shape
    count = rows // 12
    blocks = lanes // 4
    square = jax.ShapeDtypeStruct((count * 2 * blocks, blocks), jnp.float32)
    bispectrum, density, vectors, energy, mode_fields = pl.pallas_call(
        finish_kernel,
        in_specs=[VMEM],
        out_specs=[VMEM] * 5,
        out_shape=[
            square,
            square,
            jax.ShapeDtypeStruct((count, 2, blocks), jnp.float32),
            jax.ShapeDtypeStruct((1, count), jnp.float32),
            jax.ShapeDtypeStruct((count, 2, 2 * groups * lanes), jnp.float32),
        ],
        scratch_shapes=[pltpu.VMEM((8 * count, lanes), jnp.float32)],
        compiler_params=params(8),
        name="finish",
    )(got)
    whole = (count, 2, blocks, blocks)
    return (
        bispectrum.reshape(whole),
        density.reshape(whole),
        vectors,
        energy.reshape(count),
        mode_fields,
    )


def exchange(value, axis):
    return lax.all_to_all(value, axis, 0, 0, tiled=True)


def swap(value, axis, bit):
    length = lax.axis_size(axis)
    return lax.ppermute(value, axis, [(i, i ^ bit) for i in range(length)])


def local(spectra, weights, triads):
    groups = lax.axis_size("freq")
    lines = lax.axis_size("line")
    cores = lax.axis_size("core")
    f_dev, _, blocks, points = spectra.shape
    per_group = triads.shape[0] // groups
    point_count = points * lines * cores
    share = points // groups
    weights = weights.reshape(1, points)
    triads = triads.T

    send = cut(spectra.reshape(f_dev * 2 * blocks, points), groups)
    turned = exchange(send, "freq").reshape(groups * f_dev, 2 * blocks, share)

    other = sums(triads, turned, weights, groups, False)
    given = swap(other, "core", 1)
    parts = pack(sums(triads, turned, weights, groups, True), given)
    parts = exchange(parts, ("line", "freq"))

    scales = (1.0 / math.sqrt(blocks * point_count), 1.0 / point_count)
    slices = power(parts, scales, groups, lines * cores * groups)
    slices = exchange(slices, ("line", "core", "freq"))
    got = exchange(modes(triads, turned, slices, groups), "freq")
    return finish(got)


def solution(mesh):
    pts, freq = mesh.devices.shape
    finer = Mesh(mesh.devices.reshape(pts // 2, 2, freq), ("line", "core", "freq"))
    place = ("line", "core")
    in_specs = (P("freq", None, None, place), P(place), P())
    out_specs = (
        P("freq", None, None, None),
        P("freq", None, None, None),
        P("freq", None, None),
        P("freq"),
        P("freq", None, place),
    )
    return jax.shard_map(local, mesh=finer, in_specs=in_specs, out_specs=out_specs, check_vma=False)
```

```python
import math

import jax
import jax.numpy as jnp
from jax import lax
from jax.experimental import pallas as pl
from jax.experimental.pallas import tpu as pltpu
from jax.sharding import Mesh
from jax.sharding import PartitionSpec as P

ITERS = 3
EACH = 4
NT = (((1,), (1,)), ((), ()))
VMEM = pl.BlockSpec(memory_space=pltpu.VMEM)
SMEM = pl.BlockSpec(memory_space=pltpu.SMEM)


def params(mib=12):
    return pltpu.CompilerParams(vmem_limit_bytes=mib << 20)


def gram(left, right):
    half = right.shape[0] // 2
    joined = lax.dot_general(left, right, NT, preferred_element_type=jnp.float32)
    upper, lower = joined[:half], joined[half:]
    return upper + jnp.concatenate([lower[:, half:], -lower[:, :half]], axis=1)


def folded(matrix):
    half = matrix.shape[0] // 2
    return jnp.concatenate([matrix[:half], matrix[half:]], axis=1)


def cut_kernel(rows_ref, out_ref, sems):
    count, _, share = out_ref.shape
    copies = [
        pltpu.make_async_copy(
            rows_ref.at[:, pl.ds(d * share, share)], out_ref.at[d], sems.at[d]
        )
        for d in range(count)
    ]
    for copy in copies:
        copy.start()
    for copy in copies:
        copy.wait()


def cut(rows, count):
    length, points = rows.shape
    return pl.pallas_call(
        cut_kernel,
        in_specs=[pl.BlockSpec(memory_space=pltpu.HBM)],
        out_specs=VMEM,
        out_shape=pltpu.VMEM((count, length, points // count), rows.dtype),
        scratch_shapes=[pltpu.SemaphoreType.DMA((count,))],
        compiler_params=params(),
        name="cut",
    )(pltpu.with_memory_space_constraint(rows, pltpu.HBM))


def sums_kernel(groups, mine, triads_ref, spectra_ref, weights_ref, out_ref):
    total, rows, share = spectra_ref.shape
    half = rows // 2
    fold = half // 2
    count = out_ref.shape[0]
    per_group = 2 * count // groups
    core = lax.axis_index("core")
    core = core if mine else 1 - core
    offset = pl.multiple_of(lax.axis_index("freq") * share, share)

    def step(j, carry):
        t = lax.rem(j, groups) * per_group + 2 * lax.div(j, groups) + core
        k = triads_ref[0, t]
        l = triads_ref[1, t]
        m = lax.rem(k + l, total)
        first = spectra_ref[k].astype(jnp.float32)
        second = spectra_ref[l].astype(jnp.float32)
        weights = weights_ref[:, pl.ds(offset, share)]
        ar, ai, br, bi = first[:half], first[half:], second[:half], second[half:]
        re = ((ar * br - ai * bi) * weights).astype(jnp.bfloat16)
        im = ((ar * bi + ai * br) * weights).astype(jnp.bfloat16)
        product = jnp.concatenate([re, im], axis=0)
        out_ref[j, :fold] = folded(gram(product, spectra_ref[m]))
        own = spectra_ref[t]
        weighted = (own.astype(jnp.float32) * weights).astype(jnp.bfloat16)
        out_ref[j, fold:] = folded(gram(weighted, own))
        return carry

    lax.fori_loop(0, count, step, 0, unroll=32)


def sums(triads, spectra, weights, groups, mine):
    count = triads.shape[1] // 2
    total, rows, points = spectra.shape
    return pl.pallas_call(
        lambda *refs: sums_kernel(groups, mine, *refs),
        in_specs=[SMEM, VMEM, VMEM],
        out_specs=VMEM,
        out_shape=jax.ShapeDtypeStruct((count, rows // 2, 2 * rows), jnp.float32),
        cost_estimate=pl.CostEstimate(
            flops=count * rows * rows * points * 8,
            bytes_accessed=spectra.size * 2,
            transcendentals=0,
        ),
        compiler_params=params(),
        name="sums_own" if mine else "sums_other",
    )(triads, spectra, weights)


def pack_kernel(one_ref, two_ref, out_ref):
    fold = one_ref.shape[1] // 2

    def step(j, carry):
        both = one_ref[j] + two_ref[j]
        high = both[:fold].astype(jnp.bfloat16)
        rest = both[:fold] - high.astype(jnp.float32)
        out_ref[j, :fold] = high
        out_ref[j, fold : 2 * fold] = rest.astype(jnp.bfloat16)
        out_ref[j, 2 * fold :] = both[fold:].astype(jnp.bfloat16)
        return carry

    lax.fori_loop(0, one_ref.shape[0], step, 0, unroll=8)


def pack(one, two):
    count, rows, lanes = one.shape
    return pl.pallas_call(
        pack_kernel,
        in_specs=[VMEM, VMEM],
        out_specs=VMEM,
        out_shape=jax.ShapeDtypeStruct((count, 3 * rows // 2, lanes), jnp.bfloat16),
        compiler_params=params(),
        name="pack",
    )(one, two)


def high_of(value):
    return value.astype(jnp.bfloat16).astype(jnp.float32)


def power_kernel(scales, groups, parts_ref, out_ref, held_ref):
    half = parts_ref.shape[1] // 3
    added = jnp.sum(parts_ref[...].astype(jnp.float32), axis=0)
    total = (added[:half] + added[half : 2 * half]) * scales[0]
    density = added[2 * half :] * scales[1]
    blocks = 2 * half
    lane = lax.broadcasted_iota(jnp.int32, (1, 4 * blocks), 1)
    lower = lane < 2 * blocks
    other = pltpu.roll(total, 2 * blocks, 1)
    both = jnp.concatenate(
        [jnp.where(lower, total, other), jnp.where(lower, other, total)], axis=0
    )
    sign = jnp.where(lax.rem(lax.div(lane, blocks), 2) == 0, 1.0, -1.0)

    def forward(one, two):
        re = jnp.sum(both * jnp.where(lower, one, 0.0), axis=1, keepdims=True)
        im = jnp.sum(both * jnp.where(lower, two, 0.0), axis=1, keepdims=True)
        return re, im

    def square(one):
        return jnp.sum(jnp.where(lower, one * one, 0.0), axis=1, keepdims=True)

    start = 1.0 / math.sqrt(blocks)
    one = jnp.where(sign > 0, start, 0.0)
    two = jnp.where(sign > 0, 0.0, start)
    for _ in range(ITERS):
        re, im = forward(one, two)
        with_re = jnp.sum(both * re, axis=0, keepdims=True)
        with_im = jnp.sum(both * im, axis=0, keepdims=True)
        one = with_re + sign * pltpu.roll(with_im, blocks, 1)
        two = with_im - sign * pltpu.roll(with_re, blocks, 1)
        factor = 1.0 / jnp.sqrt(square(one) + 1.0)
        one = one * factor
        two = two * factor
    re, im = forward(one, two)
    top = jnp.sum(re * re + im * im, axis=0, keepdims=True)
    energy = top / (blocks * (square(one) + 1.0))
    row = jnp.where(lower, one * sign, energy)
    row_high, total_high = high_of(row), high_of(total)
    row_rest, total_rest = row - row_high, total - total_high
    for g in range(groups):
        held_ref[8 * g : 8 * g + 1] = row_high
        held_ref[8 * g + 1 : 8 * g + 2] = row_rest
        held_ref[8 * g + 2 : 8 * g + 4] = total_high[2 * g : 2 * g + 2]
        held_ref[8 * g + 4 : 8 * g + 6] = total_rest[2 * g : 2 * g + 2]
        held_ref[8 * g + 6 : 8 * g + 8] = density[2 * g : 2 * g + 2]
    slices = [held_ref[8 * g : 8 * g + 8].astype(out_ref.dtype) for g in range(groups)]
    for d in range(out_ref.shape[0]):
        out_ref[d] = slices[d % groups]


def power(parts, scales, groups, count):
    _, rows, lanes = parts.shape
    assert rows == 6 * groups
    return pl.pallas_call(
        lambda *refs: power_kernel(scales, groups, *refs),
        in_specs=[VMEM],
        out_specs=VMEM,
        out_shape=jax.ShapeDtypeStruct((count, 8, lanes), jnp.bfloat16),
        scratch_shapes=[pltpu.VMEM((8 * groups, lanes), jnp.float32)],
        compiler_params=params(8),
        name="power",
    )(parts)


def modes_kernel(triads_ref, spectra_ref, slices_ref, out_ref, pairs_ref, wide_ref, vectors_ref):
    total = spectra_ref.shape[0]
    count, height, lanes = slices_ref.shape
    groups = out_ref.shape[0]
    per_group = count // groups
    blocks = lanes // 4
    wide_ref[...] = slices_ref[...].astype(jnp.float32).reshape(count * height, lanes)
    for g in range(groups):
        vectors_ref[g * per_group : (g + 1) * per_group] = wide_ref[
            pl.ds(g * height, per_group, stride=groups * height), :
        ]
    lane = lax.broadcasted_iota(jnp.int32, (1, lanes), 1)
    lower = lane < 2 * blocks
    sign = jnp.where(lax.rem(lax.div(lane, blocks), 2) == 0, 1.0, -1.0)
    rows = jnp.where(lower, vectors_ref[...], 0.0)
    rows = rows + pltpu.roll(rows, 2 * blocks, 1)
    swapped = pltpu.roll(rows, blocks, 1)
    odd = lax.rem(lax.broadcasted_iota(jnp.int32, (count, 1), 0), 2) == 1
    keep = lower != odd
    pairs_ref[pl.ds(0, count, stride=2), :] = jnp.where(keep, rows * sign, 0.0)
    pairs_ref[pl.ds(1, count, stride=2), :] = jnp.where(keep, swapped, 0.0)
    early = lax.broadcasted_iota(jnp.int32, (2 * EACH, 1), 0) < EACH
    steps = per_group // EACH
    after = 2 * steps * 2 * EACH
    for g in range(groups):
        for s in range(steps):
            picked = []
            for q in range(EACH):
                t = g * per_group + s * EACH + q
                m = lax.rem(triads_ref[0, t] + triads_ref[1, t], total)
                picked.append(spectra_ref[m])
            right = jnp.concatenate(picked, axis=0)
            pair = pairs_ref[pl.ds(2 * (g * per_group + s * EACH), 2 * EACH), :]
            left = jnp.concatenate(
                [jnp.where(early, pair, 0.0), jnp.where(early, 0.0, pair)], axis=1
            ).astype(jnp.bfloat16)
            mixed = jnp.dot(left, right, preferred_element_type=jnp.float32)
            mixed = mixed.astype(out_ref.dtype)
            for h in range(2):
                at = (h * steps + s) * 2 * EACH
                out_ref[g, at : at + 2 * EACH] = mixed[:, h * lanes : (h + 1) * lanes]
        for k in range(2, height):
            at = after + (k - 2) * per_group
            part = wide_ref[pl.ds(g * height + k, per_group, stride=groups * height), :]
            out_ref[g, at : at + per_group] = part.astype(out_ref.dtype)


def modes(triads, spectra, slices, groups):
    count, height, lanes = slices.shape
    total, rows, points = spectra.shape
    assert points == 2 * lanes
    per_group = count // groups
    return pl.pallas_call(
        modes_kernel,
        in_specs=[SMEM, VMEM, VMEM],
        out_specs=VMEM,
        out_shape=jax.ShapeDtypeStruct((groups, (2 + height) * per_group, lanes), jnp.bfloat16),
        scratch_shapes=[
            pltpu.VMEM((2 * count, lanes), jnp.float32),
            pltpu.VMEM((count * height, lanes), jnp.float32),
            pltpu.VMEM((count, lanes), jnp.float32),
        ],
        cost_estimate=pl.CostEstimate(
            flops=count * rows * points * 4,
            bytes_accessed=spectra.size * 2,
            transcendentals=0,
        ),
        compiler_params=params(),
        name="modes",
    )(triads, spectra, slices)


def finish_kernel(
    got_ref, slices_ref, bis_ref, dens_ref, vec_ref, energy_ref, modes_ref, bis, dens, fields, held, sems
):
    groups, _, lanes = got_ref.shape
    count = modes_ref.shape[0]
    blocks = lanes // 4
    fold = blocks // 2
    first = 4 * count

    def spread(value, row, to_ref):
        for part in range(4):
            low, ri = part // 2, part % 2
            at = ri * blocks + low * fold + row
            piece = value[:, part * blocks : (part + 1) * blocks]
            to_ref[pl.ds(at, count, stride=2 * blocks), :] = piece

    for g in range(groups):
        parts = [
            got_ref[g, first + k * count : first + (k + 1) * count].astype(jnp.float32)
            for k in range(6)
        ]
        for r in range(2):
            spread(parts[r] + parts[2 + r], 2 * g + r, bis)
            spread(parts[4 + r], 2 * g + r, dens)
    copies = [
        pltpu.make_async_copy(bis, bis_ref, sems.at[0]),
        pltpu.make_async_copy(dens, dens_ref, sems.at[1]),
        pltpu.make_async_copy(fields, modes_ref, sems.at[2]),
    ]
    copies[0].start()
    copies[1].start()
    for g in range(groups):
        for h in range(2):
            block = got_ref[g, h * 2 * count : (h + 1) * 2 * count].astype(jnp.float32)
            at = (2 * g + h) * lanes
            for t in range(count):
                fields[t, :, at : at + lanes] = block[2 * t : 2 * t + 2]
    copies[2].start()

    group = lax.axis_index("freq")
    for t in range(count):
        own = slices_ref[t * groups + group].astype(jnp.float32)
        held[t : t + 1] = own[0:1] + own[1:2]
    rows = held[...]
    for t in range(count):
        for ri in range(2):
            vec_ref[t, ri : ri + 1, :] = rows[t : t + 1, ri * blocks : (ri + 1) * blocks]
    lane = lax.broadcasted_iota(jnp.int32, rows.shape, 1)
    index = lax.broadcasted_iota(jnp.int32, rows.shape, 0)
    own = jnp.where(lane == index + 2 * blocks, rows, 0.0)
    line = pltpu.roll(jnp.sum(own, axis=0, keepdims=True), 2 * blocks, 1)
    energy_ref[...] = line[:, :count]
    for copy in copies:
        copy.wait()


def finish(got, slices):
    groups, rows, lanes = got.shape
    count = rows // 10
    blocks = lanes // 4
    square = (count * 2 * blocks, blocks)
    wide = (count, 2, 2 * groups * lanes)
    there = pl.BlockSpec(memory_space=pltpu.HBM)
    bispectrum, density, vectors, energy, mode_fields = pl.pallas_call(
        finish_kernel,
        in_specs=[VMEM, VMEM],
        out_specs=[there, there, VMEM, VMEM, there],
        out_shape=[
            jax.ShapeDtypeStruct(square, jnp.float32),
            jax.ShapeDtypeStruct(square, jnp.float32),
            jax.ShapeDtypeStruct((count, 2, blocks), jnp.float32),
            jax.ShapeDtypeStruct((1, count), jnp.float32),
            jax.ShapeDtypeStruct(wide, jnp.float32),
        ],
        scratch_shapes=[
            pltpu.VMEM(square, jnp.float32),
            pltpu.VMEM(square, jnp.float32),
            pltpu.VMEM(wide, jnp.float32),
            pltpu.VMEM((count, lanes), jnp.float32),
            pltpu.SemaphoreType.DMA((3,)),
        ],
        compiler_params=params(8),
        name="finish",
    )(got, slices)
    whole = (count, 2, blocks, blocks)
    return (
        bispectrum.reshape(whole),
        density.reshape(whole),
        vectors,
        energy.reshape(count),
        mode_fields,
    )


def exchange(value, axis):
    return lax.all_to_all(value, axis, 0, 0, tiled=True)


def swap(value, axis, bit):
    length = lax.axis_size(axis)
    return lax.ppermute(value, axis, [(i, i ^ bit) for i in range(length)])


def local(spectra, weights, triads):
    groups = lax.axis_size("freq")
    lines = lax.axis_size("line")
    cores = lax.axis_size("core")
    f_dev, _, blocks, points = spectra.shape
    per_group = triads.shape[0] // groups
    point_count = points * lines * cores
    share = points // groups
    weights = weights.reshape(1, points)
    triads = triads.T

    send = cut(spectra.reshape(f_dev * 2 * blocks, points), groups)
    turned = exchange(send, "freq").reshape(groups * f_dev, 2 * blocks, share)

    other = sums(triads, turned, weights, groups, False)
    given = swap(other, "core", 1)
    parts = pack(sums(triads, turned, weights, groups, True), given)
    parts = exchange(parts, ("line", "freq"))

    scales = (1.0 / math.sqrt(blocks * point_count), 1.0 / point_count)
    slices = power(parts, scales, groups, lines * cores * groups)
    slices = exchange(slices, ("line", "core", "freq"))
    got = exchange(modes(triads, turned, slices, groups), "freq")
    return finish(got, slices)


def solution(mesh):
    pts, freq = mesh.devices.shape
    finer = Mesh(mesh.devices.reshape(pts // 2, 2, freq), ("line", "core", "freq"))
    place = ("line", "core")
    in_specs = (P("freq", None, None, place), P(place), P())
    out_specs = (
        P("freq", None, None, None),
        P("freq", None, None, None),
        P("freq", None, None),
        P("freq"),
        P("freq", None, place),
    )
    return jax.shard_map(local, mesh=finer, in_specs=in_specs, out_specs=out_specs, check_vma=False)
```

```python
import math

import jax
import jax.numpy as jnp
from jax import lax
from jax.experimental import pallas as pl
from jax.experimental.pallas import tpu as pltpu
from jax.sharding import Mesh
from jax.sharding import PartitionSpec as P

ITERS = 3
EACH = 4
STEP = 24
NT = (((1,), (1,)), ((), ()))
VMEM = pl.BlockSpec(memory_space=pltpu.VMEM)
SMEM = pl.BlockSpec(memory_space=pltpu.SMEM)


def params(mib=12):
    return pltpu.CompilerParams(vmem_limit_bytes=mib << 20)


def gram(left, right):
    half = right.shape[0] // 2
    joined = lax.dot_general(left, right, NT, preferred_element_type=jnp.float32)
    upper, lower = joined[:half], joined[half:]
    return upper + jnp.concatenate([lower[:, half:], -lower[:, :half]], axis=1)


def folded(matrix):
    half = matrix.shape[0] // 2
    return jnp.concatenate([matrix[:half], matrix[half:]], axis=1)


def cut_kernel(rows_ref, out_ref, sems):
    count, _, share = out_ref.shape
    copies = [
        pltpu.make_async_copy(
            rows_ref.at[:, pl.ds(d * share, share)], out_ref.at[d], sems.at[d]
        )
        for d in range(count)
    ]
    for copy in copies:
        copy.start()
    for copy in copies:
        copy.wait()


def cut(rows, count):
    length, points = rows.shape
    return pl.pallas_call(
        cut_kernel,
        in_specs=[pl.BlockSpec(memory_space=pltpu.HBM)],
        out_specs=VMEM,
        out_shape=pltpu.VMEM((count, length, points // count), rows.dtype),
        scratch_shapes=[pltpu.SemaphoreType.DMA((count,))],
        compiler_params=params(),
        name="cut",
    )(pltpu.with_memory_space_constraint(rows, pltpu.HBM))


def sums_kernel(groups, mine, triads_ref, spectra_ref, weights_ref, out_ref):
    total, rows, share = spectra_ref.shape
    half = rows // 2
    fold = half // 2
    count = out_ref.shape[0]
    per_group = 2 * count // groups
    core = lax.axis_index("core")
    core = core if mine else 1 - core
    offset = pl.multiple_of(lax.axis_index("freq") * share, share)

    def step(j, carry):
        t = lax.rem(j, groups) * per_group + 2 * lax.div(j, groups) + core
        k = triads_ref[0, t]
        l = triads_ref[1, t]
        m = lax.rem(k + l, total)
        first = spectra_ref[k].astype(jnp.float32)
        second = spectra_ref[l].astype(jnp.float32)
        weights = weights_ref[:, pl.ds(offset, share)]
        ar, ai, br, bi = first[:half], first[half:], second[:half], second[half:]
        re = ((ar * br - ai * bi) * weights).astype(jnp.bfloat16)
        im = ((ar * bi + ai * br) * weights).astype(jnp.bfloat16)
        product = jnp.concatenate([re, im], axis=0)
        out_ref[j, :fold] = folded(gram(product, spectra_ref[m]))
        own = spectra_ref[t]
        weighted = (own.astype(jnp.float32) * weights).astype(jnp.bfloat16)
        out_ref[j, fold:] = folded(gram(weighted, own))
        return carry

    lax.fori_loop(0, count, step, 0, unroll=32)


def sums(triads, spectra, weights, groups, mine):
    count = triads.shape[1] // 2
    total, rows, points = spectra.shape
    return pl.pallas_call(
        lambda *refs: sums_kernel(groups, mine, *refs),
        in_specs=[SMEM, VMEM, VMEM],
        out_specs=VMEM,
        out_shape=jax.ShapeDtypeStruct((count, rows // 2, 2 * rows), jnp.float32),
        cost_estimate=pl.CostEstimate(
            flops=count * rows * rows * points * 8,
            bytes_accessed=spectra.size * 2,
            transcendentals=0,
        ),
        compiler_params=params(),
        name="sums_own" if mine else "sums_other",
    )(triads, spectra, weights)


def pack_kernel(one_ref, two_ref, out_ref):
    fold = one_ref.shape[1] // 2

    def step(j, carry):
        both = one_ref[j] + two_ref[j]
        high = both[:fold].astype(jnp.bfloat16)
        rest = both[:fold] - high.astype(jnp.float32)
        out_ref[j, :fold] = high
        out_ref[j, fold : 2 * fold] = rest.astype(jnp.bfloat16)
        out_ref[j, 2 * fold :] = both[fold:].astype(jnp.bfloat16)
        return carry

    lax.fori_loop(0, one_ref.shape[0], step, 0, unroll=8)


def pack(one, two):
    count, rows, lanes = one.shape
    return pl.pallas_call(
        pack_kernel,
        in_specs=[VMEM, VMEM],
        out_specs=VMEM,
        out_shape=jax.ShapeDtypeStruct((count, 3 * rows // 2, lanes), jnp.bfloat16),
        compiler_params=params(),
        name="pack",
    )(one, two)


def high_of(value):
    return value.astype(jnp.bfloat16).astype(jnp.float32)


def power_kernel(scales, groups, parts_ref, out_ref, held_ref):
    half = parts_ref.shape[1] // 3
    added = jnp.sum(parts_ref[...].astype(jnp.float32), axis=0)
    total = (added[:half] + added[half : 2 * half]) * scales[0]
    density = added[2 * half :] * scales[1]
    blocks = 2 * half
    lane = lax.broadcasted_iota(jnp.int32, (1, 4 * blocks), 1)
    lower = lane < 2 * blocks
    other = pltpu.roll(total, 2 * blocks, 1)
    both = jnp.concatenate(
        [jnp.where(lower, total, other), jnp.where(lower, other, total)], axis=0
    )
    sign = jnp.where(lax.rem(lax.div(lane, blocks), 2) == 0, 1.0, -1.0)

    def forward(one, two):
        re = jnp.sum(both * jnp.where(lower, one, 0.0), axis=1, keepdims=True)
        im = jnp.sum(both * jnp.where(lower, two, 0.0), axis=1, keepdims=True)
        return re, im

    def square(one):
        return jnp.sum(jnp.where(lower, one * one, 0.0), axis=1, keepdims=True)

    start = 1.0 / math.sqrt(blocks)
    one = jnp.where(sign > 0, start, 0.0)
    two = jnp.where(sign > 0, 0.0, start)
    for _ in range(ITERS):
        re, im = forward(one, two)
        with_re = jnp.sum(both * re, axis=0, keepdims=True)
        with_im = jnp.sum(both * im, axis=0, keepdims=True)
        one = with_re + sign * pltpu.roll(with_im, blocks, 1)
        two = with_im - sign * pltpu.roll(with_re, blocks, 1)
        factor = 1.0 / jnp.sqrt(square(one) + 1.0)
        one = one * factor
        two = two * factor
    re, im = forward(one, two)
    top = jnp.sum(re * re + im * im, axis=0, keepdims=True)
    energy = top / (blocks * (square(one) + 1.0))
    row = jnp.where(lower, one * sign, energy)
    row_high, total_high = high_of(row), high_of(total)
    row_rest, total_rest = row - row_high, total - total_high
    for g in range(groups):
        held_ref[8 * g : 8 * g + 1] = row_high
        held_ref[8 * g + 1 : 8 * g + 2] = row_rest
        held_ref[8 * g + 2 : 8 * g + 4] = total_high[2 * g : 2 * g + 2]
        held_ref[8 * g + 4 : 8 * g + 6] = total_rest[2 * g : 2 * g + 2]
        held_ref[8 * g + 6 : 8 * g + 8] = density[2 * g : 2 * g + 2]
    slices = [held_ref[8 * g : 8 * g + 8].astype(out_ref.dtype) for g in range(groups)]
    for d in range(out_ref.shape[0]):
        out_ref[d] = slices[d % groups]


def power(parts, scales, groups, count):
    _, rows, lanes = parts.shape
    assert rows == 6 * groups
    return pl.pallas_call(
        lambda *refs: power_kernel(scales, groups, *refs),
        in_specs=[VMEM],
        out_specs=VMEM,
        out_shape=jax.ShapeDtypeStruct((count, 8, lanes), jnp.bfloat16),
        scratch_shapes=[pltpu.VMEM((8 * groups, lanes), jnp.float32)],
        compiler_params=params(8),
        name="power",
    )(parts)


def modes_kernel(triads_ref, spectra_ref, slices_ref, out_ref, pairs_ref, wide_ref, vectors_ref):
    total = spectra_ref.shape[0]
    count, height, lanes = slices_ref.shape
    groups = out_ref.shape[0]
    per_group = count // groups
    blocks = lanes // 4
    wide_ref[...] = slices_ref[...].astype(jnp.float32).reshape(count * height, lanes)
    for g in range(groups):
        vectors_ref[g * per_group : (g + 1) * per_group] = wide_ref[
            pl.ds(g * height, per_group, stride=groups * height), :
        ]
    lane = lax.broadcasted_iota(jnp.int32, (1, lanes), 1)
    lower = lane < 2 * blocks
    sign = jnp.where(lax.rem(lax.div(lane, blocks), 2) == 0, 1.0, -1.0)
    rows = jnp.where(lower, vectors_ref[...], 0.0)
    rows = rows + pltpu.roll(rows, 2 * blocks, 1)
    swapped = pltpu.roll(rows, blocks, 1)
    odd = lax.rem(lax.broadcasted_iota(jnp.int32, (count, 1), 0), 2) == 1
    keep = lower != odd
    pairs_ref[pl.ds(0, count, stride=2), :] = jnp.where(keep, rows * sign, 0.0)
    pairs_ref[pl.ds(1, count, stride=2), :] = jnp.where(keep, swapped, 0.0)
    early = lax.broadcasted_iota(jnp.int32, (2 * EACH, 1), 0) < EACH
    steps = per_group // EACH
    after = 2 * steps * 2 * EACH
    for g in range(groups):
        for s in range(steps):
            picked = []
            for q in range(EACH):
                t = g * per_group + s * EACH + q
                m = lax.rem(triads_ref[0, t] + triads_ref[1, t], total)
                picked.append(spectra_ref[m])
            right = jnp.concatenate(picked, axis=0)
            pair = pairs_ref[pl.ds(2 * (g * per_group + s * EACH), 2 * EACH), :]
            left = jnp.concatenate(
                [jnp.where(early, pair, 0.0), jnp.where(early, 0.0, pair)], axis=1
            ).astype(jnp.bfloat16)
            mixed = jnp.dot(left, right, preferred_element_type=jnp.float32)
            mixed = mixed.astype(out_ref.dtype)
            for h in range(2):
                at = (h * steps + s) * 2 * EACH
                out_ref[g, at : at + 2 * EACH] = mixed[:, h * lanes : (h + 1) * lanes]
        for k in range(2, height):
            at = after + (k - 2) * per_group
            part = wide_ref[pl.ds(g * height + k, per_group, stride=groups * height), :]
            out_ref[g, at : at + per_group] = part.astype(out_ref.dtype)


def modes(triads, spectra, slices, groups):
    count, height, lanes = slices.shape
    total, rows, points = spectra.shape
    assert points == 2 * lanes
    per_group = count // groups
    return pl.pallas_call(
        modes_kernel,
        in_specs=[SMEM, VMEM, VMEM],
        out_specs=VMEM,
        out_shape=jax.ShapeDtypeStruct((groups, (2 + height) * per_group, lanes), jnp.bfloat16),
        scratch_shapes=[
            pltpu.VMEM((2 * count, lanes), jnp.float32),
            pltpu.VMEM((count * height, lanes), jnp.float32),
            pltpu.VMEM((count, lanes), jnp.float32),
        ],
        cost_estimate=pl.CostEstimate(
            flops=count * rows * points * 4,
            bytes_accessed=spectra.size * 2,
            transcendentals=0,
        ),
        compiler_params=params(),
        name="modes",
    )(triads, spectra, slices)


def finish_kernel(
    got_ref, slices_ref, bis_ref, dens_ref, vec_ref, energy_ref, modes_ref, bis, dens, held
):
    groups, _, lanes = got_ref.shape
    count = modes_ref.shape[0]
    blocks = lanes // 4
    fold = blocks // 2
    first = 4 * count

    for g in range(groups):
        parts = [
            got_ref[g, first + k * count : first + (k + 1) * count].astype(jnp.float32)
            for k in range(6)
        ]
        for r in range(2):
            rows = pl.ds(2 * g + r, count, stride=STEP)
            bis[rows, :] = parts[r] + parts[2 + r]
            dens[rows, :] = parts[4 + r]
        for h in range(2):
            block = got_ref[g, h * 2 * count : (h + 1) * 2 * count].astype(jnp.float32)
            at = (2 * g + h) * lanes
            for t in range(count):
                modes_ref[t, :, at : at + lanes] = block[2 * t : 2 * t + 2]
    for t in range(count):
        for packed, to_ref in ((bis, bis_ref), (dens, dens_ref)):
            square = packed[STEP * t : STEP * t + fold]
            for part in range(4):
                low, ri = part // 2, part % 2
                piece = square[:, part * blocks : (part + 1) * blocks]
                to_ref[t, ri, low * fold : (low + 1) * fold, :] = piece

    group = lax.axis_index("freq")
    for t in range(count):
        own = slices_ref[t * groups + group].astype(jnp.float32)
        held[t : t + 1] = own[0:1] + own[1:2]
    rows = held[...]
    for t in range(count):
        for ri in range(2):
            vec_ref[t, ri : ri + 1, :] = rows[t : t + 1, ri * blocks : (ri + 1) * blocks]
    lane = lax.broadcasted_iota(jnp.int32, rows.shape, 1)
    index = lax.broadcasted_iota(jnp.int32, rows.shape, 0)
    own = jnp.where(lane == index + 2 * blocks, rows, 0.0)
    line = pltpu.roll(jnp.sum(own, axis=0, keepdims=True), 2 * blocks, 1)
    energy_ref[...] = line[:, :count]


def finish(got, slices):
    groups, rows, lanes = got.shape
    count = rows // 10
    blocks = lanes // 4
    square = jax.ShapeDtypeStruct((count, 2, blocks, blocks), jnp.float32)
    bispectrum, density, vectors, energy, mode_fields = pl.pallas_call(
        finish_kernel,
        in_specs=[VMEM, VMEM],
        out_specs=[VMEM] * 5,
        out_shape=[
            square,
            square,
            jax.ShapeDtypeStruct((count, 2, blocks), jnp.float32),
            jax.ShapeDtypeStruct((1, count), jnp.float32),
            jax.ShapeDtypeStruct((count, 2, 2 * groups * lanes), jnp.float32),
        ],
        scratch_shapes=[
            pltpu.VMEM((count * STEP, lanes), jnp.float32),
            pltpu.VMEM((count * STEP, lanes), jnp.float32),
            pltpu.VMEM((count, lanes), jnp.float32),
        ],
        compiler_params=params(8),
        name="finish",
    )(got, slices)
    return (bispectrum, density, vectors, energy.reshape(count), mode_fields)


def exchange(value, axis):
    return lax.all_to_all(value, axis, 0, 0, tiled=True)


def swap(value, axis, bit):
    length = lax.axis_size(axis)
    return lax.ppermute(value, axis, [(i, i ^ bit) for i in range(length)])


def local(spectra, weights, triads):
    groups = lax.axis_size("freq")
    lines = lax.axis_size("line")
    cores = lax.axis_size("core")
    f_dev, _, blocks, points = spectra.shape
    per_group = triads.shape[0] // groups
    point_count = points * lines * cores
    share = points // groups
    weights = weights.reshape(1, points)
    triads = triads.T

    send = cut(spectra.reshape(f_dev * 2 * blocks, points), groups)
    turned = exchange(send, "freq").reshape(groups * f_dev, 2 * blocks, share)

    other = sums(triads, turned, weights, groups, False)
    given = swap(other, "core", 1)
    parts = pack(sums(triads, turned, weights, groups, True), given)
    parts = exchange(parts, ("line", "freq"))

    scales = (1.0 / math.sqrt(blocks * point_count), 1.0 / point_count)
    slices = power(parts, scales, groups, lines * cores * groups)
    slices = exchange(slices, ("line", "core", "freq"))
    got = exchange(modes(triads, turned, slices, groups), "freq")
    return finish(got, slices)


def solution(mesh):
    pts, freq = mesh.devices.shape
    finer = Mesh(mesh.devices.reshape(pts // 2, 2, freq), ("line", "core", "freq"))
    place = ("line", "core")
    in_specs = (P("freq", None, None, place), P(place), P())
    out_specs = (
        P("freq", None, None, None),
        P("freq", None, None, None),
        P("freq", None, None),
        P("freq"),
        P("freq", None, place),
    )
    return jax.shard_map(local, mesh=finer, in_specs=in_specs, out_specs=out_specs, check_vma=False)
```

```python
import math

import jax
import jax.numpy as jnp
from jax import lax
from jax.experimental import pallas as pl
from jax.experimental.pallas import tpu as pltpu
from jax.sharding import Mesh
from jax.sharding import PartitionSpec as P

ITERS = 3
EACH = 4
STEP = 24
NT = (((1,), (1,)), ((), ()))
VMEM = pl.BlockSpec(memory_space=pltpu.VMEM)
SMEM = pl.BlockSpec(memory_space=pltpu.SMEM)


def params(mib=12):
    return pltpu.CompilerParams(vmem_limit_bytes=mib << 20)


def gram(left, right):
    half = right.shape[0] // 2
    joined = lax.dot_general(left, right, NT, preferred_element_type=jnp.float32)
    upper, lower = joined[:half], joined[half:]
    return upper + jnp.concatenate([lower[:, half:], -lower[:, :half]], axis=1)


def gram_of_itself(left, right):
    half = right.shape[0] // 2
    joined = lax.dot_general(left, right, NT, preferred_element_type=jnp.float32)
    upper, lower = joined[:half], joined[half:]
    return (upper[:, :half] - lower[:, :half]) + (upper[:, half:] + lower[:, half:])


def folded(matrix, count):
    rows = matrix.shape[0] // count
    return jnp.concatenate([matrix[k * rows : (k + 1) * rows] for k in range(count)], axis=1)


def cut_kernel(rows_ref, out_ref, sems):
    count, _, share = out_ref.shape
    copies = [
        pltpu.make_async_copy(
            rows_ref.at[:, pl.ds(d * share, share)], out_ref.at[d], sems.at[d]
        )
        for d in range(count)
    ]
    for copy in copies:
        copy.start()
    for copy in copies:
        copy.wait()


def cut(rows, count):
    length, points = rows.shape
    return pl.pallas_call(
        cut_kernel,
        in_specs=[pl.BlockSpec(memory_space=pltpu.HBM)],
        out_specs=VMEM,
        out_shape=pltpu.VMEM((count, length, points // count), rows.dtype),
        scratch_shapes=[pltpu.SemaphoreType.DMA((count,))],
        compiler_params=params(),
        name="cut",
    )(pltpu.with_memory_space_constraint(rows, pltpu.HBM))


def sums_kernel(groups, mine, triads_ref, spectra_ref, weights_ref, out_ref):
    total, rows, share = spectra_ref.shape
    half = rows // 2
    fold = half // 2
    count = out_ref.shape[0]
    per_group = 2 * count // groups
    core = lax.axis_index("core")
    core = core if mine else 1 - core
    offset = pl.multiple_of(lax.axis_index("freq") * share, share)

    def step(j, carry):
        t = lax.rem(j, groups) * per_group + 2 * lax.div(j, groups) + core
        k = triads_ref[0, t]
        l = triads_ref[1, t]
        m = lax.rem(k + l, total)
        first = spectra_ref[k].astype(jnp.float32)
        second = spectra_ref[l].astype(jnp.float32)
        weights = weights_ref[:, pl.ds(offset, share)]
        ar, ai, br, bi = first[:half], first[half:], second[:half], second[half:]
        re = ((ar * br - ai * bi) * weights).astype(jnp.bfloat16)
        im = ((ar * bi + ai * br) * weights).astype(jnp.bfloat16)
        product = jnp.concatenate([re, im], axis=0)
        out_ref[j, :fold] = folded(gram(product, spectra_ref[m]), 2)
        own = spectra_ref[t]
        weighted = (own.astype(jnp.float32) * weights).astype(jnp.bfloat16)
        out_ref[j, fold:] = folded(gram_of_itself(weighted, own), 4)
        return carry

    lax.fori_loop(0, count, step, 0, unroll=32)


def sums(triads, spectra, weights, groups, mine):
    count = triads.shape[1] // 2
    total, rows, points = spectra.shape
    return pl.pallas_call(
        lambda *refs: sums_kernel(groups, mine, *refs),
        in_specs=[SMEM, VMEM, VMEM],
        out_specs=VMEM,
        out_shape=jax.ShapeDtypeStruct((count, 3 * rows // 8, 2 * rows), jnp.float32),
        cost_estimate=pl.CostEstimate(
            flops=count * rows * rows * points * 8,
            bytes_accessed=spectra.size * 2,
            transcendentals=0,
        ),
        compiler_params=params(),
        name="sums_own" if mine else "sums_other",
    )(triads, spectra, weights)


def pack_kernel(one_ref, two_ref, out_ref):
    fold = 2 * one_ref.shape[1] // 3

    def step(j, carry):
        both = one_ref[j] + two_ref[j]
        high = both[:fold].astype(jnp.bfloat16)
        rest = both[:fold] - high.astype(jnp.float32)
        out_ref[j, :fold] = high
        out_ref[j, fold : 2 * fold] = rest.astype(jnp.bfloat16)
        out_ref[j, 2 * fold :] = both[fold:].astype(jnp.bfloat16)
        return carry

    lax.fori_loop(0, one_ref.shape[0], step, 0, unroll=8)


def pack(one, two):
    count, rows, lanes = one.shape
    return pl.pallas_call(
        pack_kernel,
        in_specs=[VMEM, VMEM],
        out_specs=VMEM,
        out_shape=jax.ShapeDtypeStruct((count, 5 * rows // 3, lanes), jnp.bfloat16),
        compiler_params=params(),
        name="pack",
    )(one, two)


def power_kernel(scales, groups, parts_ref, out_ref, held_ref):
    half = 2 * parts_ref.shape[1] // 5
    added = jnp.sum(parts_ref[...].astype(jnp.float32), axis=0)
    total = (added[:half] + added[half : 2 * half]) * scales[0]
    density = added[2 * half :] * scales[1]
    blocks = 2 * half
    lane = lax.broadcasted_iota(jnp.int32, (1, 4 * blocks), 1)
    lower = lane < 2 * blocks
    other = pltpu.roll(total, 2 * blocks, 1)
    both = jnp.concatenate(
        [jnp.where(lower, total, other), jnp.where(lower, other, total)], axis=0
    )
    sign = jnp.where(lax.rem(lax.div(lane, blocks), 2) == 0, 1.0, -1.0)

    def forward(one, two):
        re = jnp.sum(both * jnp.where(lower, one, 0.0), axis=1, keepdims=True)
        im = jnp.sum(both * jnp.where(lower, two, 0.0), axis=1, keepdims=True)
        return re, im

    def square(one):
        return jnp.sum(jnp.where(lower, one * one, 0.0), axis=1, keepdims=True)

    start = 1.0 / math.sqrt(blocks)
    one = jnp.where(sign > 0, start, 0.0)
    two = jnp.where(sign > 0, 0.0, start)
    for _ in range(ITERS):
        re, im = forward(one, two)
        with_re = jnp.sum(both * re, axis=0, keepdims=True)
        with_im = jnp.sum(both * im, axis=0, keepdims=True)
        one = with_re + sign * pltpu.roll(with_im, blocks, 1)
        two = with_im - sign * pltpu.roll(with_re, blocks, 1)
        factor = 1.0 / jnp.sqrt(square(one) + 1.0)
        one = one * factor
        two = two * factor
    re, im = forward(one, two)
    top = jnp.sum(re * re + im * im, axis=0, keepdims=True)
    energy = top / (blocks * (square(one) + 1.0))
    row = jnp.where(lower, one * sign, energy)
    for g in range(groups):
        held_ref[8 * g : 8 * g + 1] = row
        held_ref[8 * g + 1 : 8 * g + 3] = total[2 * g : 2 * g + 2]
        held_ref[8 * g + 3 : 8 * g + 4] = density[g : g + 1]
    slices = [held_ref[8 * g : 8 * g + 4].astype(out_ref.dtype) for g in range(groups)]
    for d in range(out_ref.shape[0]):
        out_ref[d] = slices[d % groups]


def power(parts, scales, groups, count):
    _, rows, lanes = parts.shape
    assert rows == 5 * groups
    return pl.pallas_call(
        lambda *refs: power_kernel(scales, groups, *refs),
        in_specs=[VMEM],
        out_specs=VMEM,
        out_shape=jax.ShapeDtypeStruct((count, 4, lanes), jnp.bfloat16),
        scratch_shapes=[pltpu.VMEM((8 * groups, lanes), jnp.float32)],
        compiler_params=params(8),
        name="power",
    )(parts)


def modes_kernel(triads_ref, spectra_ref, slices_ref, out_ref, pairs_ref, wide_ref, vectors_ref):
    total = spectra_ref.shape[0]
    count, height, lanes = slices_ref.shape
    groups = out_ref.shape[0]
    per_group = count // groups
    blocks = lanes // 4
    for d in range(count):
        wide_ref[8 * d : 8 * d + height] = slices_ref[d].astype(jnp.float32)
    for g in range(groups):
        vectors_ref[g * per_group : (g + 1) * per_group] = wide_ref[
            pl.ds(8 * g, per_group, stride=8 * groups), :
        ]
    lane = lax.broadcasted_iota(jnp.int32, (1, lanes), 1)
    lower = lane < 2 * blocks
    sign = jnp.where(lax.rem(lax.div(lane, blocks), 2) == 0, 1.0, -1.0)
    rows = jnp.where(lower, vectors_ref[...], 0.0)
    rows = rows + pltpu.roll(rows, 2 * blocks, 1)
    swapped = pltpu.roll(rows, blocks, 1)
    odd = lax.rem(lax.broadcasted_iota(jnp.int32, (count, 1), 0), 2) == 1
    keep = lower != odd
    pairs_ref[pl.ds(0, count, stride=2), :] = jnp.where(keep, rows * sign, 0.0)
    pairs_ref[pl.ds(1, count, stride=2), :] = jnp.where(keep, swapped, 0.0)
    early = lax.broadcasted_iota(jnp.int32, (2 * EACH, 1), 0) < EACH
    steps = per_group // EACH
    after = 2 * steps * 2 * EACH
    for g in range(groups):
        for s in range(steps):
            picked = []
            for q in range(EACH):
                t = g * per_group + s * EACH + q
                m = lax.rem(triads_ref[0, t] + triads_ref[1, t], total)
                picked.append(spectra_ref[m])
            right = jnp.concatenate(picked, axis=0)
            pair = pairs_ref[pl.ds(2 * (g * per_group + s * EACH), 2 * EACH), :]
            left = jnp.concatenate(
                [jnp.where(early, pair, 0.0), jnp.where(early, 0.0, pair)], axis=1
            ).astype(jnp.bfloat16)
            mixed = jnp.dot(left, right, preferred_element_type=jnp.float32)
            mixed = mixed.astype(out_ref.dtype)
            for h in range(2):
                at = (h * steps + s) * 2 * EACH
                out_ref[g, at : at + 2 * EACH] = mixed[:, h * lanes : (h + 1) * lanes]
        for k in range(1, height):
            at = after + (k - 1) * per_group
            part = wide_ref[pl.ds(8 * g + k, per_group, stride=8 * groups), :]
            out_ref[g, at : at + per_group] = part.astype(out_ref.dtype)


def modes(triads, spectra, slices, groups):
    count, height, lanes = slices.shape
    total, rows, points = spectra.shape
    assert points == 2 * lanes
    per_group = count // groups
    return pl.pallas_call(
        modes_kernel,
        in_specs=[SMEM, VMEM, VMEM],
        out_specs=VMEM,
        out_shape=jax.ShapeDtypeStruct((groups, (3 + height) * per_group, lanes), jnp.bfloat16),
        scratch_shapes=[
            pltpu.VMEM((2 * count, lanes), jnp.float32),
            pltpu.VMEM((8 * count, lanes), jnp.float32),
            pltpu.VMEM((count, lanes), jnp.float32),
        ],
        cost_estimate=pl.CostEstimate(
            flops=count * rows * points * 4,
            bytes_accessed=spectra.size * 2,
            transcendentals=0,
        ),
        compiler_params=params(),
        name="modes",
    )(triads, spectra, slices)


def finish_kernel(
    got_ref, slices_ref, bis_ref, dens_ref, vec_ref, energy_ref, modes_ref, bis, dens, held
):
    groups, _, lanes = got_ref.shape
    count = modes_ref.shape[0]
    blocks = lanes // 4
    fold = blocks // 2
    first = 4 * count

    for g in range(groups):
        parts = [
            got_ref[g, first + k * count : first + (k + 1) * count].astype(jnp.float32)
            for k in range(3)
        ]
        for r in range(2):
            bis[pl.ds(2 * g + r, count, stride=STEP), :] = parts[r]
        dens[pl.ds(g, count, stride=groups), :] = parts[2]
        for h in range(2):
            block = got_ref[g, h * 2 * count : (h + 1) * 2 * count].astype(jnp.float32)
            at = (2 * g + h) * lanes
            for t in range(count):
                modes_ref[t, :, at : at + lanes] = block[2 * t : 2 * t + 2]
    for t in range(count):
        square = bis[STEP * t : STEP * t + fold]
        for part in range(4):
            low, ri = part // 2, part % 2
            piece = square[:, part * blocks : (part + 1) * blocks]
            bis_ref[t, ri, low * fold : (low + 1) * fold, :] = piece
    for t in range(0, count, 4):
        runs = []
        for q in range(4):
            pieces = [
                dens[groups * (t + k) : groups * (t + k + 1), q * blocks : (q + 1) * blocks]
                for k in range(4)
            ]
            runs.append(jnp.concatenate(pieces, axis=1))
        four = jnp.concatenate(runs, axis=0)
        turned = four.T
        for k in range(4):
            square = four[:, k * blocks : (k + 1) * blocks]
            other = turned[k * blocks : (k + 1) * blocks, :]
            dens_ref[t + k, 0] = 0.5 * (square + other)
            dens_ref[t + k, 1] = 0.5 * (square - other)

    group = lax.axis_index("freq")
    for t in range(count):
        held[t : t + 1] = slices_ref[t * groups + group].astype(jnp.float32)[0:1]
    rows = held[...]
    for t in range(count):
        for ri in range(2):
            vec_ref[t, ri : ri + 1, :] = rows[t : t + 1, ri * blocks : (ri + 1) * blocks]
    lane = lax.broadcasted_iota(jnp.int32, rows.shape, 1)
    index = lax.broadcasted_iota(jnp.int32, rows.shape, 0)
    own = jnp.where(lane == index + 2 * blocks, rows, 0.0)
    line = pltpu.roll(jnp.sum(own, axis=0, keepdims=True), 2 * blocks, 1)
    energy_ref[...] = line[:, :count]


def finish(got, slices):
    groups, rows, lanes = got.shape
    count = rows // 7
    blocks = lanes // 4
    square = jax.ShapeDtypeStruct((count, 2, blocks, blocks), jnp.float32)
    bispectrum, density, vectors, energy, mode_fields = pl.pallas_call(
        finish_kernel,
        in_specs=[VMEM, VMEM],
        out_specs=[VMEM] * 5,
        out_shape=[
            square,
            square,
            jax.ShapeDtypeStruct((count, 2, blocks), jnp.float32),
            jax.ShapeDtypeStruct((1, count), jnp.float32),
            jax.ShapeDtypeStruct((count, 2, 2 * groups * lanes), jnp.float32),
        ],
        scratch_shapes=[
            pltpu.VMEM((count * STEP, lanes), jnp.float32),
            pltpu.VMEM((count * groups, lanes), jnp.float32),
            pltpu.VMEM((count, lanes), jnp.float32),
        ],
        compiler_params=params(8),
        name="finish",
    )(got, slices)
    return (bispectrum, density, vectors, energy.reshape(count), mode_fields)


def exchange(value, axis):
    return lax.all_to_all(value, axis, 0, 0, tiled=True)


def swap(value, axis, bit):
    length = lax.axis_size(axis)
    return lax.ppermute(value, axis, [(i, i ^ bit) for i in range(length)])


def local(spectra, weights, triads):
    groups = lax.axis_size("freq")
    lines = lax.axis_size("line")
    cores = lax.axis_size("core")
    f_dev, _, blocks, points = spectra.shape
    per_group = triads.shape[0] // groups
    point_count = points * lines * cores
    share = points // groups
    weights = weights.reshape(1, points)
    triads = triads.T

    send = cut(spectra.reshape(f_dev * 2 * blocks, points), groups)
    turned = exchange(send, "freq").reshape(groups * f_dev, 2 * blocks, share)

    other = sums(triads, turned, weights, groups, False)
    given = swap(other, "core", 1)
    parts = pack(sums(triads, turned, weights, groups, True), given)
    parts = exchange(parts, ("line", "freq"))

    scales = (1.0 / math.sqrt(blocks * point_count), 1.0 / point_count)
    slices = power(parts, scales, groups, lines * cores * groups)
    slices = exchange(slices, ("line", "core", "freq"))
    got = exchange(modes(triads, turned, slices, groups), "freq")
    return finish(got, slices)


def solution(mesh):
    pts, freq = mesh.devices.shape
    finer = Mesh(mesh.devices.reshape(pts // 2, 2, freq), ("line", "core", "freq"))
    place = ("line", "core")
    in_specs = (P("freq", None, None, place), P(place), P())
    out_specs = (
        P("freq", None, None, None),
        P("freq", None, None, None),
        P("freq", None, None),
        P("freq"),
        P("freq", None, place),
    )
    return jax.shard_map(local, mesh=finer, in_specs=in_specs, out_specs=out_specs, check_vma=False)
```
